128 devices in a mesh: dp: 64 (over z, y, x), fsdp: 2 (over core).
Axes of the slice: x: 4, y: 4, z: 4, core: 2. Of those that a mesh axis runs over, the one named last changes fastest.
Arguments:
- tokens: int32 [256, 768], P(('dp', 'fsdp'))
- grad_y: bfloat16 [256, 768, 768], P(('dp', 'fsdp'))
- embedding: bfloat16 [33, 768], P(None, 'fsdp')
- ln1_gain: bfloat16 [768], P('fsdp')
- ln1_bias: bfloat16 [768], P('fsdp')
- w_qkv: bfloat16 [768, 2304], P('fsdp')
- b_qkv: bfloat16 [2304], P('fsdp')
- w_out: bfloat16 [768, 768], P('fsdp')
- b_out: bfloat16 [768], P('fsdp')
- ln2_gain: bfloat16 [768], P('fsdp')
- ln2_bias: bfloat16 [768], P('fsdp')
- w_fc1: bfloat16 [768, 3072], P('fsdp')
- b_fc1: bfloat16 [3072], P('fsdp')
- w_fc2: bfloat16 [3072, 768], P('fsdp')
- b_fc2: bfloat16 [768], P('fsdp')
Outputs:
- output 1: bfloat16 [256, 768, 768], P(('dp', 'fsdp'))
- output 2: float32 [33, 768], P(None, 'fsdp')
- output 3: float32 [768], P('fsdp')
- output 4: float32 [768], P('fsdp')
- output 5: float32 [768, 2304], P('fsdp')
- output 6: float32 [2304], P('fsdp')
- output 7: float32 [768, 768], P('fsdp')
- output 8: float32 [768], P('fsdp')
- output 9: float32 [768], P('fsdp')
- output 10: float32 [768], P('fsdp')
- output 11: float32 [768, 3072], P('fsdp')
- output 12: float32 [3072], P('fsdp')
- output 13: float32 [3072, 768], P('fsdp')
- output 14: float32 [768], P('fsdp')
All inputs are finite; a program needn't handle non-finite values.
Results may differ from the reference program's by a relative error of at most 0.0118225.
Values are sent between devices in bfloat16 or wider.
A program may use at most 1 GiB of HBM per device.

```python
import jax
import jax.numpy as jnp
from jax import lax

D = 768
HEADS = 12
FF = 3072
SEQ = 768
BATCH = 256
VOCAB = 33
CLS_ID = 0
PAD_ID = 1
EOS_ID = 2
MASK_ID = 32

HEAD_DIM = D // HEADS
MASK_RATIO = 0.15 * 0.8
LN_EPS = 1e-5
ROPE_BASE = 10000.0


def draw_tokens(tok_key):
    len_key, res_key, rate_key, pick_key = jax.random.split(tok_key, 4)
    lengths = jax.random.randint(len_key, (BATCH,), SEQ // 2, SEQ + 1)
    lengths = lengths.at[0].set(SEQ).at[1].set(SEQ // 2)
    position = jnp.arange(SEQ)[None, :]
    residues = jax.random.randint(res_key, (BATCH, SEQ), 4, 29)
    mask_rate = jax.random.randint(rate_key, (BATCH, 1), 5, 26)
    pick_draw = jax.random.randint(pick_key, (BATCH, SEQ), 0, 100)
    body_tok = jnp.where(pick_draw < mask_rate, MASK_ID, residues)
    last_pos = lengths[:, None] - 1
    tok_grid = jnp.where(position < last_pos, body_tok, PAD_ID)
    tok_grid = jnp.where(position == last_pos, EOS_ID, tok_grid)
    return jnp.where(position == 0, CLS_ID, tok_grid).astype(jnp.int32)


def setup_inputs(seed: int = 0) -> dict:
    keys = jax.random.split(jax.random.key(seed), 16)

    def draw_normal(sub_key, dims, std_scale, offset=0.0):
        return (jax.random.normal(sub_key, dims, jnp.float32) * std_scale + offset).astype(jnp.bfloat16)

    return {
        'tokens': draw_tokens(keys[0]),
        'grad_y': draw_normal(keys[1], (BATCH, SEQ, D), 1.0),
        'embedding': draw_normal(keys[2], (VOCAB, D), 1.0),
        'ln1_gain': draw_normal(keys[3], (D,), 0.2, 1.0),
        'ln1_bias': draw_normal(keys[4], (D,), 0.2),
        'w_qkv': draw_normal(keys[5], (D, 3 * D), D ** -0.5),
        'b_qkv': draw_normal(keys[6], (3 * D,), 0.2),
        'w_out': draw_normal(keys[7], (D, D), D ** -0.5),
        'b_out': draw_normal(keys[8], (D,), 0.2),
        'ln2_gain': draw_normal(keys[9], (D,), 0.2, 1.0),
        'ln2_bias': draw_normal(keys[10], (D,), 0.2),
        'w_fc1': draw_normal(keys[11], (D, FF), D ** -0.5),
        'b_fc1': draw_normal(keys[12], (FF,), 0.2),
        'w_fc2': draw_normal(keys[13], (FF, D), FF ** -0.5),
        'b_fc2': draw_normal(keys[14], (D,), 0.2),
    }


def to_bf16(x_val):
    return x_val.astype(jnp.bfloat16).astype(jnp.float32)


def mat_mul(lhs, rhs):
    return jnp.dot(lhs, rhs, preferred_element_type=jnp.float32)


def layer_norm(x_val, gain, bias):
    centered = x_val - jnp.mean(x_val, axis=-1, keepdims=True)
    row_var = jnp.mean(centered * centered, axis=-1, keepdims=True)
    return centered * lax.rsqrt(row_var + LN_EPS) * gain + bias


def rope_tables():
    inv_freq = 1.0 / (ROPE_BASE ** (jnp.arange(0, HEAD_DIM, 2, dtype=jnp.float32) / HEAD_DIM))
    angles = jnp.arange(SEQ, dtype=jnp.float32)[:, None] * inv_freq[None, :]
    return jnp.cos(angles)[:, None, :], jnp.sin(angles)[:, None, :]


def rotate(x_val, cos_tab, sin_tab):
    half_dim = x_val.shape[-1] // 2
    low_half = x_val[..., :half_dim]
    high_half = x_val[..., half_dim:]
    return jnp.concatenate([low_half * cos_tab - high_half * sin_tab, high_half * cos_tab + low_half * sin_tab], axis=-1)


def seq_forward(weights, tok_row):
    (embedding, ln1_gain, ln1_bias, w_qkv, b_qkv, w_out, b_out,
     ln2_gain, ln2_bias, w_fc1, b_fc1, w_fc2, b_fc2) = weights
    is_mask = tok_row == MASK_ID
    is_pad = tok_row == PAD_ID
    mask_count = jnp.sum(is_mask.astype(jnp.float32))
    real_count = jnp.sum(jnp.logical_not(is_pad).astype(jnp.float32))
    factor = (1.0 - MASK_RATIO) / (1.0 - mask_count / real_count)
    keep_scale = jnp.where(is_mask | is_pad, 0.0, factor)
    x_in = to_bf16(embedding[tok_row] * keep_scale[:, None])
    h_one = to_bf16(layer_norm(x_in, ln1_gain, ln1_bias))
    qkv_proj = (mat_mul(h_one, w_qkv) + b_qkv).reshape(SEQ, 3, HEADS, HEAD_DIM)
    cos_tab, sin_tab = rope_tables()
    queries = to_bf16(rotate(qkv_proj[:, 0] * HEAD_DIM ** -0.5, cos_tab, sin_tab))
    key_rows = to_bf16(rotate(qkv_proj[:, 1], cos_tab, sin_tab))
    values = to_bf16(qkv_proj[:, 2])
    scores = jnp.einsum('qhd,khd->hqk', queries, key_rows)
    scores = jnp.where(is_pad[None, None, :], -1e30, scores)
    attn_prob = to_bf16(jax.nn.softmax(scores, axis=-1))
    context = to_bf16(jnp.einsum('hqk,khd->qhd', attn_prob, values)).reshape(SEQ, D)
    x_mid = x_in + mat_mul(context, w_out) + b_out
    h_two = to_bf16(layer_norm(x_mid, ln2_gain, ln2_bias))
    hidden_act = to_bf16(jax.nn.gelu(mat_mul(h_two, w_fc1) + b_fc1, approximate=False))
    return to_bf16(x_mid + mat_mul(hidden_act, w_fc2) + b_fc2)


def reference(tokens, grad_y, embedding, ln1_gain, ln1_bias, w_qkv, b_qkv, w_out, b_out,
              ln2_gain, ln2_bias, w_fc1, b_fc1, w_fc2, b_fc2):
    weights = tuple(w.astype(jnp.float32) for w in (embedding, ln1_gain, ln1_bias, w_qkv, b_qkv, w_out, b_out,
                                                     ln2_gain, ln2_bias, w_fc1, b_fc1, w_fc2, b_fc2))
    grad_init = tuple(jnp.zeros_like(w) for w in weights)

    def scan_step(grad_sum, seq_pair):
        tok_row, dy_row = seq_pair
        y_row, pull_back = jax.vjp(lambda params: seq_forward(params, tok_row), weights)
        grad_row = pull_back(dy_row.astype(jnp.float32))[0]
        new_sum = tuple(a_sum + g_row for a_sum, g_row in zip(grad_sum, grad_row))
        return new_sum, y_row.astype(jnp.bfloat16)

    grad_total, hidden = lax.scan(scan_step, grad_init, (tokens, grad_y))
    return (hidden,) + tuple(grad_total)
```

```python
import functools
import jax
import jax.numpy as jnp
from jax import lax
from jax.experimental import pallas as pl
from jax.experimental.pallas import tpu as pltpu
from jax.sharding import PartitionSpec as P

HEAD_DIM = 64
MASK_ID = 32
PAD_ID = 1
MASK_RATIO = 0.15 * 0.8
LN_EPS = 1e-5
ROPE_BASE = 10000.0
F32 = jnp.float32
BF16 = jnp.bfloat16
VOCAB_ROWS = 48
VMEM_LIMIT = 60 * 1024 * 1024

NN = (((1,), (0,)), ((), ()))
NT = (((1,), (1,)), ((), ()))
TN = (((0,), (0,)), ((), ()))


def dot(lhs, rhs, dims=NN):
    return lax.dot_general(lhs, rhs, dims, preferred_element_type=F32)


def hat_of(x_val):
    centered = x_val - jnp.mean(x_val, axis=-1, keepdims=True)
    inv_std = lax.rsqrt(jnp.mean(centered * centered, axis=-1, keepdims=True) + LN_EPS)
    return centered * inv_std, inv_std


def hat_bwd(d_out, x_hat, inv_std, gain):
    d_hat = d_out * gain
    return inv_std * (d_hat - jnp.mean(d_hat, axis=-1, keepdims=True)
                      - x_hat * jnp.mean(d_hat * x_hat, axis=-1, keepdims=True))


def rope_tables(seq_len):
    inv_freq = 1.0 / (ROPE_BASE ** (jnp.arange(0, HEAD_DIM, 2, dtype=F32) / HEAD_DIM))
    angles = jnp.arange(seq_len, dtype=F32)[:, None] * inv_freq[None, :]
    cos, sin = jnp.cos(angles), jnp.sin(angles)
    return jnp.concatenate([cos] * 4, axis=1), jnp.concatenate([-sin, sin] * 2, axis=1)


def swap_halves(x_val):
    lane = lax.broadcasted_iota(jnp.int32, x_val.shape, 1)
    low = (lane & 32) == 0
    return jnp.where(low, pltpu.roll(x_val, 96, 1), pltpu.roll(x_val, 32, 1))


def rows_of_head(x_val, head):
    row = lax.broadcasted_iota(jnp.int32, x_val.shape, 0)
    return jnp.where((row >= 64) == (head == 1), x_val, jnp.zeros_like(x_val))


def lanes_of_head(x_val, head):
    lane = lax.broadcasted_iota(jnp.int32, x_val.shape, 1)
    return jnp.where((lane >= 64) == (head == 1), x_val, jnp.zeros_like(x_val))


def qkv_kernel(tok, keep, emb, gain, bias, w_qkv, b_qkv, cos, sin, x_out, q_out, k_out, v_out):
    dim = x_out.shape[1]
    one_hot = (tok[...] == lax.broadcasted_iota(jnp.int32, (tok.shape[0], emb.shape[0]), 1))
    looked_up = dot(one_hot.astype(F32).astype(BF16), emb[...])
    x_b16 = (looked_up * keep[...]).astype(BF16)
    x_out[...] = x_b16
    x_hat, _ = hat_of(x_b16.astype(F32))
    h_one = (x_hat * gain[...] + bias[...]).astype(BF16)
    cos_tab, sin_tab = cos[...], sin[...]
    for part, out in enumerate((q_out, k_out, v_out)):
        cols = slice(part * dim, (part + 1) * dim)
        proj = dot(h_one, w_qkv[:, cols]) + b_qkv[:, cols]
        if part == 0:
            proj = proj * HEAD_DIM ** -0.5
        if part < 2:
            for pair in range(dim // 128):
                z = proj[:, pair * 128:(pair + 1) * 128]
                out[:, pair * 128:(pair + 1) * 128] = (z * cos_tab + swap_halves(z) * sin_tab).astype(BF16)
        else:
            out[...] = proj.astype(BF16)


CHUNK = 256


def attn_fwd_kernel(q, k, v, pad, ctx, lse):
    q_t = q[...].T
    v_t = v[...].T
    k_val = k[...]
    pad_tab = jnp.concatenate([pad[...]] * (CHUNK // 128), axis=1)
    for c in range(q.shape[0] // CHUNK):
        cols = slice(c * CHUNK, (c + 1) * CHUNK)
        parts = []
        for head in range(2):
            s_t = dot(k_val, rows_of_head(q_t[:, cols], head)) + pad_tab
            top = jnp.max(s_t, axis=0, keepdims=True)
            e_t = jnp.exp(s_t - top)
            total = jnp.sum(e_t, axis=0, keepdims=True)
            lse[0, head:head + 1, cols] = top + jnp.log(total)
            p_t = (e_t * (1.0 / total)).astype(BF16)
            parts.append(dot(v_t[head * 64:(head + 1) * 64, :], p_t))
        ctx[cols, :] = jnp.concatenate(parts, axis=0).T.astype(BF16)


def attn_bwd_kernel(q, k, v, d_ctx, lse, pad, cos, sin, dq_out, dk_out, dv_out, sums, dk_acc, dv_acc):
    q_val, k_val, v_val, d_val = q[...], k[...], v[...], d_ctx[...]
    q_t, k_t, d_t = q_val.T, k_val.T, d_val.T
    pad_tab = jnp.concatenate([pad[...]] * (CHUNK // 128), axis=1)
    dq_sum = jnp.zeros((1, 128), F32)
    for c in range(q.shape[0] // CHUNK):
        cols = slice(c * CHUNK, (c + 1) * CHUNK)
        parts = []
        for head in range(2):
            s_t = dot(k_val, rows_of_head(q_t[:, cols], head)) + pad_tab
            p_t = jnp.exp(s_t - lse[0, head:head + 1, cols])
            dp_t = dot(v_val, rows_of_head(d_t[:, cols], head))
            delta = jnp.sum(p_t * dp_t, axis=0, keepdims=True)
            ds_t = (p_t * (dp_t - delta)).astype(BF16)
            dv_new = dot(p_t.astype(BF16), lanes_of_head(d_val[cols, :], head))
            dk_new = dot(ds_t, lanes_of_head(q_val[cols, :], head))
            if c == 0 and head == 0:
                dv_acc[...] = dv_new
                dk_acc[...] = dk_new
            else:
                dv_acc[...] += dv_new
                dk_acc[...] += dk_new
            parts.append(dot(k_t[head * 64:(head + 1) * 64, :], ds_t))
        z = jnp.concatenate(parts, axis=0).T
        z = (z * cos[cols, :] - swap_halves(z) * sin[cols, :]) * HEAD_DIM ** -0.5
        dq_sum = dq_sum + jnp.sum(z, axis=0, keepdims=True)
        dq_out[cols, :] = z.astype(BF16)
    z = dk_acc[...]
    z = z * cos[...] - swap_halves(z) * sin[...]
    dk_out[...] = z.astype(BF16)
    z_v = dv_acc[...]
    dv_out[...] = z_v.astype(BF16)
    sums[0, 0:1, :] = dq_sum
    sums[0, 1:2, :] = jnp.sum(z, axis=0, keepdims=True)
    sums[0, 2:3, :] = jnp.sum(z_v, axis=0, keepdims=True)


FF_CHUNK = 768


def accumulate(ref, index, value, first):
    @pl.when(first)
    def _():
        ref[index] = value

    @pl.when(jnp.logical_not(first))
    def _():
        ref[index] += value


def ffn_kernel(ctx, x_in, grad_y, w_out, w_fc1, w_fc2, b_out, gain, bias, b_fc1, b_fc2,
               y_out, dmid_out, dctx_out, gw_out, gw_fc1, gw_fc2, g_small, g_b1, y_acc, dh_acc):
    step = pl.program_id(0)
    @pl.when(step == 0)
    def _():
        for ref in (gw_out, gw_fc1, gw_fc2, g_small, g_b1):
            ref[...] = jnp.zeros_like(ref)

    ctx_val = ctx[...]
    x_mid = x_in[...].astype(F32) + dot(ctx_val, w_out[...]) + b_out[...]
    x_hat, inv_std = hat_of(x_mid)
    h_two = (x_hat * gain[...] + bias[...]).astype(BF16)
    dy = grad_y[...]
    y_acc[...] = x_mid + b_fc2[...]
    for j in range(w_fc1.shape[1] // FF_CHUNK):
        cols = slice(j * FF_CHUNK, (j + 1) * FF_CHUNK)
        pre = dot(h_two, w_fc1[:, cols]) + b_fc1[:, cols]
        cdf = 0.5 + 0.5 * lax.erf(pre * (0.5 ** 0.5))
        pdf = jnp.exp(pre * pre * -0.5) * 0.3989422804014327
        act = (pre * cdf).astype(BF16)
        d_act = dot(dy, w_fc2[cols, :], NT)
        d_pre = d_act * (cdf + pre * pdf)
        y_acc[...] += dot(act, w_fc2[cols, :])
        gw_fc2[cols, :] += dot(act, dy, TN)
        g_b1[:, cols] += jnp.sum(d_pre, axis=0, keepdims=True)
        d_pre = d_pre.astype(BF16)
        gw_fc1[j] += dot(h_two, d_pre, TN)
        d_h = dot(d_pre, w_fc1[:, cols], NT)
        if j == 0:
            dh_acc[...] = d_h
        else:
            dh_acc[...] += d_h
    y_out[...] = y_acc[...].astype(BF16)
    d_two = dh_acc[...]
    dy_f = dy.astype(F32)
    g_small[0:1, :] += jnp.sum(dy_f, axis=0, keepdims=True)
    g_small[1:2, :] += jnp.sum(d_two * x_hat, axis=0, keepdims=True)
    g_small[2:3, :] += jnp.sum(d_two, axis=0, keepdims=True)
    d_mid = dy_f + hat_bwd(d_two, x_hat, inv_std, gain[...])
    dmid_out[...] = d_mid
    g_small[3:4, :] += jnp.sum(d_mid, axis=0, keepdims=True)
    d_mid = d_mid.astype(BF16)
    gw_out[...] += dot(ctx_val, d_mid, TN)
    dctx_out[...] = dot(d_mid, w_out[...], NT).astype(BF16)


def qkv_bwd_kernel(tok_row, keep, x_in, dq, dk, dv, d_mid, w_qkv, gain, bias, gw_qkv, g_emb, g_small):
    step = pl.program_id(0)
    @pl.when(step == 0)
    def _():
        for ref in (gw_qkv, g_emb, g_small):
            ref[...] = jnp.zeros_like(ref)

    dim = x_in.shape[1]
    x_hat, inv_std = hat_of(x_in[...].astype(F32))
    h_one = (x_hat * gain[...] + bias[...]).astype(BF16)
    d_one = None
    for part, ref in enumerate((dq, dk, dv)):
        cols = slice(part * dim, (part + 1) * dim)
        d_part = ref[...]
        gw_qkv[part] += dot(h_one, d_part, TN)
        new = dot(d_part, w_qkv[:, cols], NT)
        d_one = new if part == 0 else d_one + new
    g_small[0:1, :] += jnp.sum(d_one * x_hat, axis=0, keepdims=True)
    g_small[1:2, :] += jnp.sum(d_one, axis=0, keepdims=True)
    d_in = (d_mid[...] + hat_bwd(d_one, x_hat, inv_std, gain[...])) * keep[...]
    one_hot = (tok_row[0] == lax.broadcasted_iota(jnp.int32, (g_emb.shape[0], d_in.shape[0]), 0))
    one_hot = one_hot.astype(F32).astype(BF16)
    high = d_in.astype(BF16)
    low = (d_in - high.astype(F32)).astype(BF16)
    g_emb[...] += dot(one_hot, high) + dot(one_hot, low)


def whole(shape):
    return pl.BlockSpec(shape, lambda *_: (0,) * len(shape), pipeline_mode=pl.Buffered(1))


def shape_of(dims, dtype):
    return jax.ShapeDtypeStruct(dims, dtype)


def call(kernel, grid, in_specs, out_specs, out_shape, args, flops, scratch=(), name=None):
    moved = sum(a.size * a.dtype.itemsize for a in args) + sum(o.size * o.dtype.itemsize for o in out_shape)
    return pl.pallas_call(
        kernel, grid=grid, in_specs=in_specs, out_specs=out_specs, out_shape=out_shape,
        scratch_shapes=list(scratch), name=name,
        compiler_params=pltpu.CompilerParams(vmem_limit_bytes=VMEM_LIMIT,
                                             dimension_semantics=('arbitrary',) * len(grid)),
        cost_estimate=pl.CostEstimate(flops=flops, bytes_accessed=moved, transcendentals=0))(*args)


def layer_compute(tokens, grad_y, small, w_qkv, w_out, w_fc1, w_fc2):
    (embedding, ln1_gain, ln1_bias, b_qkv, b_out, ln2_gain, ln2_bias, b_fc1, b_fc2) = small
    rows, seq_len = tokens.shape
    dim = embedding.shape[1]
    ff = w_fc1.shape[1]
    n_tok = rows * seq_len
    pairs = dim // 128

    is_mask = tokens == MASK_ID
    is_pad = tokens == PAD_ID
    mask_count = jnp.sum(is_mask, axis=1).astype(F32)
    real_count = jnp.sum(jnp.logical_not(is_pad), axis=1).astype(F32)
    factor = (1.0 - MASK_RATIO) / (1.0 - mask_count / real_count)
    keep = jnp.where(is_mask | is_pad, 0.0, factor[:, None]).reshape(n_tok, 1)
    pad_tab = jnp.broadcast_to(jnp.where(is_pad, -1e30, 0.0).astype(F32).reshape(n_tok, 1), (n_tok, 128))
    tok_col = tokens.reshape(n_tok, 1)
    cos, sin = rope_tables(seq_len)
    emb_pad = jnp.pad(embedding, ((0, VOCAB_ROWS - embedding.shape[0]), (0, 0)))

    def row(vec):
        return vec.astype(F32).reshape(1, -1)

    g1, c1, g2, c2 = row(ln1_gain), row(ln1_bias), row(ln2_gain), row(ln2_bias)

    tile = 256
    per_seq = seq_len // tile
    tile_spec = lambda width: pl.BlockSpec((tile, width), lambda i: (i, 0))
    seq_spec = pl.BlockSpec((tile, 128), lambda i: (i % per_seq, 0))
    x_in, q, k, v = call(
        qkv_kernel, (n_tok // tile,),
        [tile_spec(1), tile_spec(1), whole(emb_pad.shape), whole((1, dim)), whole((1, dim)),
         whole(w_qkv.shape), whole((1, 3 * dim)), seq_spec, seq_spec],
        [tile_spec(dim)] * 4, [shape_of((n_tok, dim), BF16)] * 4,
        (tok_col, keep, emb_pad, g1, c1, w_qkv, row(b_qkv), cos, sin), 2 * n_tok * dim * 3 * dim, name='qkv')

    head_spec = pl.BlockSpec((seq_len, 128), lambda b, p: (b, p))
    pad_spec = pl.BlockSpec((seq_len, 128), lambda b, p: (b, 0))
    lse_spec = pl.BlockSpec((1, 2, seq_len), lambda b, p: (b * pairs + p, 0, 0))
    ctx, lse = call(
        attn_fwd_kernel, (rows, pairs), [head_spec] * 3 + [pad_spec], [head_spec, lse_spec],
        [shape_of((n_tok, dim), BF16), shape_of((rows * pairs, 2, seq_len), F32)],
        (q, k, v, pad_tab), 16 * n_tok * seq_len * dim, name='attn_fwd')

    tile = 512
    tile_spec3 = lambda width: pl.BlockSpec((tile, width), lambda i: (i, 0))
    hidden, d_mid, d_ctx, gw_out, gw_fc1, gw_fc2, small_two, g_b1 = call(
        ffn_kernel, (n_tok // tile,),
        [tile_spec3(dim)] * 3 + [whole(w.shape) for w in (w_out, w_fc1, w_fc2)]
        + [whole((1, dim))] * 3 + [whole((1, ff)), whole((1, dim))],
        [tile_spec3(dim)] * 3 + [whole(w_out.shape), whole((ff // dim, dim, dim)), whole(w_fc2.shape)]
        + [whole((8, dim)), whole((1, ff))],
        [shape_of((n_tok, dim), BF16), shape_of((n_tok, dim), F32), shape_of((n_tok, dim), BF16),
         shape_of(w_out.shape, F32), shape_of((ff // dim, dim, dim), F32), shape_of(w_fc2.shape, F32),
         shape_of((8, dim), F32), shape_of((1, ff), F32)],
        (ctx, x_in, grad_y.reshape(n_tok, dim), w_out, w_fc1, w_fc2, row(b_out), g2, c2, row(b_fc1), row(b_fc2)),
        2 * n_tok * dim * (3 * dim + 6 * ff),
        scratch=[pltpu.VMEM((tile, dim), F32), pltpu.VMEM((tile, dim), F32)], name='ffn')

    tab_spec = pl.BlockSpec((seq_len, 128), lambda b, p: (0, 0))
    dq, dk, dv, sums = call(
        attn_bwd_kernel, (rows, pairs),
        [head_spec] * 4 + [lse_spec, pad_spec, tab_spec, tab_spec],
        [head_spec] * 3 + [pl.BlockSpec((1, 3, 128), lambda b, p: (b * pairs + p, 0, 0))],
        [shape_of((n_tok, dim), BF16)] * 3 + [shape_of((rows * pairs, 3, 128), F32)],
        (q, k, v, d_ctx, lse, pad_tab, cos, sin), 40 * n_tok * seq_len * dim,
        scratch=[pltpu.VMEM((seq_len, 128), F32)] * 2, name='attn_bwd')

    gw_qkv, g_emb, small_one = call(
        qkv_bwd_kernel, (n_tok // tile,),
        [pl.BlockSpec((1, 1, tile), lambda i: (i, 0, 0)), tile_spec3(1)] + [tile_spec3(dim)] * 5
        + [whole(w_qkv.shape), whole((1, dim)), whole((1, dim))],
        [whole((3, dim, dim)), whole((VOCAB_ROWS, dim)), whole((8, dim))],
        [shape_of((3, dim, dim), F32), shape_of((VOCAB_ROWS, dim), F32), shape_of((8, dim), F32)],
        (tokens.reshape(n_tok // tile, 1, tile), keep, x_in, dq, dk, dv, d_mid, w_qkv, g1, c1),
        4 * n_tok * dim * 3 * dim, name='qkv_bwd')
    g_b_qkv = jnp.sum(sums.reshape(rows, pairs, 3, 128), axis=0).transpose(1, 0, 2).reshape(3 * dim)
    small_grads = (g_emb[:embedding.shape[0]], small_one[0], small_one[1], g_b_qkv, small_two[3],
                   small_two[1], small_two[2], g_b1[0], small_two[0])
    return hidden.reshape(grad_y.shape), small_grads, (gw_qkv, gw_out, gw_fc1, gw_fc2)


RING = 4
ORDERS = ('xyz', 'yzx', 'zxy')
STRIDE = {'x': 1, 'y': RING, 'z': RING * RING}
MESH_ID = pl.DeviceIdType.MESH


class Torus:
    def __init__(self):
        self.me = lax.axis_index('dp')
        self.part = lax.axis_index('fsdp')
        self.coord = {axis: self.me // stride % RING for axis, stride in STRIDE.items()}

    def at(self, axis, delta):
        return (self.coord[axis] + delta + RING) % RING

    def chip(self, axis, delta):
        return {'dp': self.me + (self.at(axis, delta) - self.coord[axis]) * STRIDE[axis]}

    def partner(self):
        return {'fsdp': 1 - self.part}

    def greet(self):
        barrier = pltpu.get_barrier_semaphore()
        peers = [self.partner()] + [self.chip(axis, delta) for axis in 'xyz' for delta in (1, -1)]
        for peer in peers:
            pl.semaphore_signal(barrier, inc=1, device_id=peer, device_id_type=MESH_ID)
        pl.semaphore_wait(barrier, len(peers))


class Flow:
    def __init__(self, torus, order, sign, view, temp_view, grads, sums, temps, sends, recvs, base):
        self.torus, self.order, self.sign = torus, order, sign
        self.view, self.temp_view = view, temp_view
        self.grads, self.sums, self.temps = grads, sums, temps
        self.sends, self.recvs, self.base = sends, recvs, base
        self.copies = {}

    def start(self, slot, src, dst, level, delta):
        copy = pltpu.make_async_remote_copy(
            src_ref=src, dst_ref=dst, send_sem=self.sends.at[self.base + slot], recv_sem=self.recvs.at[self.base + slot],
            device_id=self.torus.chip(self.order[level], delta), device_id_type=MESH_ID)
        copy.start()
        self.copies[slot] = copy

    def place(self, level, delta=None):
        own = [self.torus.coord[axis] for axis in self.order[:level]]
        return tuple(own) + (() if delta is None else (self.torus.at(self.order[level], delta),))

    def scatter_start(self, level):
        sign, slot = self.sign, level * 3
        self.start(slot, self.view(self.grads, self.place(level, 2)), self.temp_view(self.temps, level, 0), level, sign)
        self.start(slot + 1, self.view(self.grads, self.place(level, -sign)), self.temp_view(self.temps, level, 1),
                   level, -sign)

    def scatter_mid(self, level):
        slot = level * 3
        self.copies[slot].wait_recv()
        relay = self.temp_view(self.temps, level, 0)
        relay[...] = relay[...] + self.view(self.grads, self.place(level, self.sign))[...]
        self.start(slot + 2, relay, self.temp_view(self.temps, level, 2), level, self.sign)

    def scatter_end(self, level):
        slot = level * 3
        self.copies[slot + 1].wait_recv()
        self.copies[slot + 2].wait_recv()
        mine = self.view(self.grads, self.place(level, 0))
        total = mine[...] + self.temp_view(self.temps, level, 1)[...] + self.temp_view(self.temps, level, 2)[...]
        mine[...] = total
        if level == 2:
            self.view(self.sums, self.place(3))[...] = total

    def gather_start(self, level):
        sign, slot = self.sign, 9 + level * 3
        src = self.view(self.grads if level == 2 else self.sums, self.place(level + 1))
        dst = self.view(self.sums, self.place(level + 1))
        self.start(slot, src, dst, level, sign)
        self.start(slot + 1, src, dst, level, -sign)

    def gather_mid(self, level):
        slot = 9 + level * 3
        self.copies[slot].wait_recv()
        block = self.view(self.sums, self.place(level, -self.sign))
        self.start(slot + 2, block, block, level, self.sign)

    def gather_end(self, level):
        slot = 9 + level * 3
        self.copies[slot + 1].wait_recv()
        self.copies[slot + 2].wait_recv()

    def finish(self):
        for copy in self.copies.values():
            copy.wait_send()


FLOW_SEMS = 18


def big_flows(torus, width, grads, sums, temps, sends, recvs, base):
    half = width // 2
    flows = []
    for color, order in enumerate(ORDERS):
        for side, sign in enumerate((1, -1)):
            lanes = pl.ds(side * half, half)

            def view(ref, place, color=color, lanes=lanes):
                rest = place[1:] + (slice(None),) * (4 - len(place))
                return ref.at[(place[0], slice(None), color) + rest + (lanes,)]

            def temp_view(refs, level, kind, color=color, lanes=lanes):
                return refs[level].at[(kind, slice(None), color) + (slice(None),) * (3 - level) + (lanes,)]

            flows.append(Flow(torus, order, sign, view, temp_view, grads, sums, temps, sends, recvs,
                              base + len(flows) * FLOW_SEMS))
    return flows


def small_flow(torus, grads, sums, temps, sends, recvs, base):
    def view(ref, place):
        return ref.at[place + (slice(None),) * (5 - len(place))]

    def temp_view(refs, level, kind):
        return refs[level].at[kind]

    return Flow(torus, ORDERS[0], 1, view, temp_view, grads, sums, temps, sends, recvs, base)


def all_reduce_steps(flows):
    steps = [lambda: [f.scatter_start(0) for f in flows]]
    for level in range(3):
        def mid(level=level):
            for f in flows:
                f.scatter_mid(level)

        def end(level=level):
            for f in flows:
                f.scatter_end(level)
                if level < 2:
                    f.scatter_start(level + 1)
                else:
                    f.gather_start(2)
        steps += [mid, end]
    for level in (2, 1, 0):
        def mid(level=level):
            for f in flows:
                f.gather_mid(level)

        def end(level=level):
            for f in flows:
                f.gather_end(level)
                if level > 0:
                    f.gather_start(level - 1)
        steps += [mid, end]
    return steps


def reduce_kernel(fc2, fc1, out, qkv, small, fc2_sum, fc1_sum, out_sum, qkv_sum, small_sum,
                  grads, sums, temp0, temp1, temp2, s_grads, s_sums, s_temp0, s_temp1, s_temp2,
                  sends, recvs, local):
    torus = Torus()
    width = grads.shape[-1]
    torus.greet()
    part, other = torus.part, 1 - torus.part
    pieces = [
        (lambda i: fc2.at[i], lambda ref: ref.at[:, 0]),
        (lambda i: fc1.at[:, i], lambda ref: ref.at[:, 1]),
        (lambda i: out.at[i], lambda ref: ref.at[0, 2]),
        (lambda i: qkv.at[:, i], lambda ref: ref.at[1:4, 2]),
    ]
    copies = []
    for n, (source, place) in enumerate(pieces):
        copies.append((pltpu.make_async_remote_copy(
            src_ref=source(other), dst_ref=place(sums), send_sem=sends.at[n], recv_sem=recvs.at[n],
            device_id=torus.partner(), device_id_type=MESH_ID),
            pltpu.make_async_copy(source(part), place(grads), local.at[n])))
    copies.append((pltpu.make_async_remote_copy(
        src_ref=small.at[other], dst_ref=s_sums, send_sem=sends.at[4], recv_sem=recvs.at[4],
        device_id=torus.partner(), device_id_type=MESH_ID),
        pltpu.make_async_copy(small.at[part], s_grads, local.at[4])))
    for remote, mine in copies:
        remote.start()
        mine.start()
    for n, (remote, mine) in enumerate(copies):
        remote.wait_recv()
        mine.wait()
        if n < 4:
            dst, src = pieces[n][1](grads), pieces[n][1](sums)
        else:
            dst, src = s_grads, s_sums

        @pl.loop(0, dst.shape[0])
        def _(i):
            dst[i] = dst[i] + src[i]
    flows = big_flows(torus, width, grads, sums, (temp0, temp1, temp2), sends, recvs, 5)
    flows.append(small_flow(torus, s_grads, s_sums, (s_temp0, s_temp1, s_temp2), sends, recvs, 5 + 6 * FLOW_SEMS))
    for step in all_reduce_steps(flows):
        step()
    stores = [
        pltpu.make_async_copy(sums.at[:, 0], fc2_sum, local.at[0]),
        pltpu.make_async_copy(sums.at[0, 2], out_sum, local.at[2]),
        pltpu.make_async_copy(s_sums, small_sum, local.at[4]),
    ]
    for page in range(RING):
        lanes = pl.ds(page * width, width)
        stores.append(pltpu.make_async_copy(sums.at[page, 1], fc1_sum.at[:, :, :, :, lanes], local.at[5 + page]))
        if page < 3:
            stores.append(pltpu.make_async_copy(sums.at[page + 1, 2], qkv_sum.at[:, :, :, :, lanes], local.at[9 + page]))
    for store in stores:
        store.start()
    for remote, _ in copies:
        remote.wait_send()
    for flow in flows:
        flow.finish()
    for store in stores:
        store.wait()


def reduce_gradients(gw_qkv, gw_out, gw_fc1, gw_fc2, small):
    dim = gw_out.shape[1]
    rows = dim // 2
    blocks = (3, RING, RING, rows // (3 * RING * RING), dim)
    temps = [pltpu.VMEM((3, 3, 3) + (RING,) * (2 - level) + (blocks[3], dim), F32) for level in range(3)]
    s_temps = [pltpu.VMEM((3,) + (RING,) * (2 - level) + (8, 128), F32) for level in range(3)]
    n_sems = 5 + 7 * FLOW_SEMS
    outs = [shape_of((4,) + blocks, F32), shape_of(blocks[:4] + (4 * dim,), F32), shape_of(blocks, F32),
            shape_of(blocks[:4] + (3 * dim,), F32), shape_of((RING, RING, RING, 8, 128), F32)]
    any_spec = pl.BlockSpec(memory_space=pl.ANY)
    fc2, fc1, out, qkv, small_sum = pl.pallas_call(
        reduce_kernel, in_specs=[any_spec] * 5, out_specs=[any_spec] * 5, out_shape=outs, name='reduce',
        scratch_shapes=[pltpu.VMEM((RING, 3) + blocks, F32)] * 2 + temps
        + [pltpu.VMEM((RING, RING, RING, 8, 128), F32)] * 2 + s_temps
        + [pltpu.SemaphoreType.DMA((n_sems,)), pltpu.SemaphoreType.DMA((n_sems,)), pltpu.SemaphoreType.DMA((12,))],
        compiler_params=pltpu.CompilerParams(vmem_limit_bytes=VMEM_LIMIT, collective_id=0, has_side_effects=True),
    )(gw_fc2.reshape((2, 4) + blocks), gw_fc1.reshape((4, 2) + blocks), gw_out.reshape((2,) + blocks),
      gw_qkv.reshape((3, 2) + blocks), small)
    return (qkv.reshape(rows, 3 * dim), out.reshape(rows, dim), fc1.reshape(rows, 4 * dim),
            fc2.reshape(4 * rows, dim), small_sum)


def solution(mesh):
    row_spec = P(('dp', 'fsdp'), None)
    act_spec = P(('dp', 'fsdp'), None, None)
    param_specs = (P(None, 'fsdp'),) + (P('fsdp'),) * 12
    n_part = mesh.shape['fsdp']

    def local_step(tokens, grad_y, *shards):
        (embedding, ln1_gain, ln1_bias, w_qkv, b_qkv, w_out, b_out,
         ln2_gain, ln2_bias, w_fc1, b_fc1, w_fc2, b_fc2) = shards
        vectors = (ln1_gain, ln1_bias, b_qkv, b_out, ln2_gain, ln2_bias, b_fc1, b_fc2)
        vocab, part_dim = embedding.shape
        packed = jnp.concatenate([embedding.reshape(-1)] + list(vectors))
        packed = lax.all_gather(packed, 'fsdp', axis=0)
        full = [packed[:, :vocab * part_dim].reshape(n_part, vocab, part_dim).transpose(1, 0, 2).reshape(vocab, -1)]
        start = vocab * part_dim
        for vec in vectors:
            full.append(packed[:, start:start + vec.size].reshape(-1))
            start += vec.size
        full_w = [lax.all_gather(w, 'fsdp', axis=0, tiled=True) for w in (w_qkv, w_out, w_fc1, w_fc2)]
        hidden, small_grads, big_grads = layer_compute(tokens, grad_y, full, *full_w)

        flat = jnp.concatenate(
            [small_grads[0].reshape(vocab, n_part, part_dim).transpose(1, 0, 2).reshape(n_part, -1)]
            + [g.reshape(n_part, -1) for g in small_grads[1:]], axis=1)
        flat = jnp.pad(flat, ((0, 0), (0, RING ** 3 * 1024 - flat.shape[1])))
        *summed, small_sum = reduce_gradients(*big_grads, flat.reshape(n_part, RING, RING, RING, 8, 128))
        mine = small_sum.reshape(-1)
        g_embedding = mine[:vocab * part_dim].reshape(vocab, part_dim)
        start = vocab * part_dim
        vec_grads = []
        for vec in vectors:
            vec_grads.append(mine[start:start + vec.size])
            start += vec.size
        (g_ln1_gain, g_ln1_bias, g_b_qkv, g_b_out, g_ln2_gain, g_ln2_bias, g_b_fc1, g_b_fc2) = vec_grads
        g_w_qkv, g_w_out, g_w_fc1, g_w_fc2 = summed
        return (hidden, g_embedding, g_ln1_gain, g_ln1_bias, g_w_qkv, g_b_qkv, g_w_out, g_b_out,
                g_ln2_gain, g_ln2_bias, g_w_fc1, g_b_fc1, g_w_fc2, g_b_fc2)

    return jax.shard_map(local_step, mesh=mesh, in_specs=(row_spec, act_spec) + param_specs,
                         out_specs=(act_spec,) + param_specs, check_vma=False)
```

```python
import functools
import jax
import jax.numpy as jnp
import numpy as np
from jax import lax
from jax.experimental import pallas as pl
from jax.experimental.pallas import tpu as pltpu
from jax.sharding import PartitionSpec as P

HEAD_DIM = 64
MASK_ID = 32
PAD_ID = 1
MASK_RATIO = 0.15 * 0.8
LN_EPS = 1e-5
ROPE_BASE = 10000.0
F32 = jnp.float32
BF16 = jnp.bfloat16
EMB_ROWS = 40
SMALL_ROWS = 64
VEC_ROW = 48
VECTORS = ('ln1_gain', 'ln1_bias', 'b_out', 'ln2_gain', 'ln2_bias', 'b_fc2', 'b_qkv', 'b_fc1')
VMEM_LIMIT = 60 << 20

NN = (((1,), (0,)), ((), ()))
NT = (((1,), (1,)), ((), ()))
TN = (((0,), (0,)), ((), ()))


def dot(lhs, rhs, dims=NN):
    return lax.dot_general(lhs, rhs, dims, preferred_element_type=F32)


def row_mean(x_val):
    return jnp.mean(x_val, axis=-1, keepdims=True)


def hat_of(x_val):
    centered = x_val - row_mean(x_val)
    inv_std = lax.rsqrt(row_mean(centered * centered) + LN_EPS)
    return centered * inv_std, inv_std


def hat_bwd(d_out, x_hat, inv_std, gain):
    d_hat = d_out * gain
    return inv_std * (d_hat - row_mean(d_hat)
                      - x_hat * row_mean(d_hat * x_hat))


def rope_tables(seq_len):
    power = np.arange(0, HEAD_DIM, 2, dtype=np.float32) / np.float32(HEAD_DIM)
    inv_freq = np.float32(1) / np.power(np.float32(ROPE_BASE), power)
    angles = np.outer(np.arange(seq_len, dtype=np.float32), inv_freq).astype(np.float64)
    cos, sin = np.cos(angles), np.sin(angles)
    return (jnp.asarray(np.concatenate([cos] * 4, axis=1), F32),
            jnp.asarray(np.concatenate([-sin, sin] * 2, axis=1), F32))


def col_sum(x_val):
    return jnp.sum(x_val, axis=0, keepdims=True)


def iota(shape, dim):
    return lax.broadcasted_iota(jnp.int32, shape, dim)


def vec_row(vec, name):
    at = VECTORS.index(name)
    count = {'b_qkv': 3, 'b_fc1': 4}.get(name, 1)
    row = VEC_ROW + at + (2 if name == 'b_fc1' else 0)
    return jnp.concatenate([vec[side, i:i + 1, :] for side in range(2) for i in range(row, row + count)],
                           axis=1).astype(F32)


def seq_counts(tok_row):
    masks = jnp.sum((tok_row == MASK_ID).astype(F32), axis=1, keepdims=True)
    real = jnp.sum((tok_row != PAD_ID).astype(F32), axis=1, keepdims=True)
    return (1.0 - MASK_RATIO) / (1.0 - masks / real), real


def live_one_hot(tok_row, rows):
    live = (tok_row == iota((rows, tok_row.shape[1]), 0)) & (tok_row != MASK_ID) & (tok_row != PAD_ID)
    return live.astype(F32).astype(BF16)


def swap_halves(x_val):
    low = (iota(x_val.shape, 1) & 32) == 0
    return jnp.where(low, pltpu.roll(x_val, 96, 1), pltpu.roll(x_val, 32, 1))


def rows_of_head(x_val, head):
    return jnp.where((iota(x_val.shape, 0) >= HEAD_DIM) == (head == 1), x_val, jnp.zeros_like(x_val))


def lanes_of_head(x_val, head):
    return jnp.where((iota(x_val.shape, 1) >= HEAD_DIM) == (head == 1), x_val, jnp.zeros_like(x_val))


def qkv_kernel(tok_seq, tok_tile, vec_part, cos, sin, wq_part, wo_part, w1_part, w2_part,
               x_out, q_out, k_out, v_out, vec_out, wq_out, wo_out, w1_out, w2_out,
               w_qkv, vec, wo_own, w1_own, w2_own, sends, recvs, local):
    step = pl.program_id(0)
    part = lax.axis_index('fsdp')
    partner = {'fsdp': 1 - part}
    dim = x_out.shape[1]

    def own_rows(ref):
        size = ref.shape[0] // 2
        return ref.at[pl.ds(part * size, size)]

    moves = [(wq_part, w_qkv), (vec_part, vec.at[part]), (wo_own, wo_out), (w1_own, w1_out), (w2_own, w2_out)]

    def target(n):
        return moves[n][1] if n == 1 else own_rows(moves[n][1])

    def remote(n):
        return pltpu.make_async_remote_copy(
            src_ref=moves[n][0], dst_ref=target(n), send_sem=sends.at[n], recv_sem=recvs.at[n],
            device_id=partner, device_id_type=MESH_ID)

    def keep_own(n):
        return pltpu.make_async_copy(moves[n][0], target(n), local.at[n])

    stage = ((wo_part, wo_own), (w1_part, w1_own), (w2_part, w2_own))

    def store_qkv():
        return pltpu.make_async_copy(w_qkv, wq_out, local.at[len(moves) + len(stage)])

    @pl.when(step == 0)
    def _():
        barrier = pltpu.get_barrier_semaphore()
        pl.semaphore_signal(barrier, inc=1, device_id=partner, device_id_type=MESH_ID)
        pl.semaphore_wait(barrier, 1)
        for n in range(2):
            remote(n).start()
            keep_own(n).start()
        loads = [pltpu.make_async_copy(src, dst, local.at[len(moves) + n]) for n, (src, dst) in enumerate(stage)]
        for copy in loads:
            copy.start()
        for n, copy in enumerate(loads):
            copy.wait()
            remote(n + 2).start()
            keep_own(n + 2).start()
        for n in range(2):
            remote(n).wait_recv()
            keep_own(n).wait()
        store_qkv().start()
        vec_out[...] = vec[...]

    scale, _ = seq_counts(tok_seq[0])
    emb = jnp.concatenate([vec[side, :VEC_ROW, :] for side in range(2)], axis=1)
    x_b16 = (dot(live_one_hot(tok_tile[0], VEC_ROW), emb, TN) * scale).astype(BF16)
    x_out[...] = x_b16
    x_hat, _ = hat_of(x_b16.astype(F32))
    h_one = (x_hat * vec_row(vec, 'ln1_gain') + vec_row(vec, 'ln1_bias')).astype(BF16)
    cos_tab, sin_tab = cos[...], sin[...]
    b_qkv = vec_row(vec, 'b_qkv')
    for index, out in enumerate((q_out, k_out, v_out)):
        cols = slice(index * dim, (index + 1) * dim)
        proj = dot(h_one, w_qkv[:, cols]) + b_qkv[:, cols]
        if out is v_out:
            out[...] = proj.astype(BF16)
            continue
        if out is q_out:
            proj = proj * HEAD_DIM ** -0.5
        for first in range(0, dim, PAIR):
            pair = slice(first, first + PAIR)
            z = proj[:, pair]
            out[:, pair] = (z * cos_tab + swap_halves(z) * sin_tab).astype(BF16)

    @pl.when(step == pl.num_programs(0) - 1)
    def _():
        store_qkv().wait()
        for n in range(len(moves)):
            remote(n).wait_send()
            if n >= 2:
                remote(n).wait_recv()
                keep_own(n).wait()


PAIR = 2 * HEAD_DIM
CHUNK = 256


def pad_bias(tok_row, keys):
    _, real = seq_counts(tok_row)
    return jnp.where(iota((keys, CHUNK), 0).astype(F32) < real, 0.0, -1e30)


def attn_fwd_kernel(q, k, v, tok_seq, ctx, lse):
    q_t = q[...].T
    v_t = v[...].T
    k_val = k[...]
    pad_tab = pad_bias(tok_seq[0], q.shape[0])
    for c in range(q.shape[0] // CHUNK):
        cols = slice(c * CHUNK, (c + 1) * CHUNK)
        parts = []
        for head in range(2):
            s_t = dot(k_val, rows_of_head(q_t[:, cols], head)) + pad_tab
            top = jnp.max(s_t, axis=0, keepdims=True)
            e_t = jnp.exp(s_t - top)
            total = col_sum(e_t)
            lse[0, head:head + 1, cols] = top + jnp.log(total)
            p_t = (e_t * (1.0 / total)).astype(BF16)
            parts.append(dot(v_t[head * HEAD_DIM:(head + 1) * HEAD_DIM, :], p_t))
        ctx[cols, :] = jnp.concatenate(parts, axis=0).T.astype(BF16)


def attn_bwd_kernel(q, k, v, d_ctx, lse, tok_seq, cos, sin, dq_out, dk_out, dv_out, sums, dk_acc, dv_acc):
    q_val, k_val, v_val, d_val = q[...], k[...], v[...], d_ctx[...]
    q_t, k_t, d_t = q_val.T, k_val.T, d_val.T
    pad_tab = pad_bias(tok_seq[0], q.shape[0])
    dq_sum = jnp.zeros((1, 128), F32)
    for c in range(q.shape[0] // CHUNK):
        cols = slice(c * CHUNK, (c + 1) * CHUNK)
        parts = []
        for head in range(2):
            s_t = dot(k_val, rows_of_head(q_t[:, cols], head)) + pad_tab
            p_t = jnp.exp(s_t - lse[0, head:head + 1, cols])
            dp_t = dot(v_val, rows_of_head(d_t[:, cols], head))
            delta = col_sum(p_t * dp_t)
            ds_t = (p_t * (dp_t - delta)).astype(BF16)
            dv_new = dot(p_t.astype(BF16), lanes_of_head(d_val[cols, :], head))
            dk_new = dot(ds_t, lanes_of_head(q_val[cols, :], head))
            if c == 0 and head == 0:
                dv_acc[...] = dv_new
                dk_acc[...] = dk_new
            else:
                dv_acc[...] += dv_new
                dk_acc[...] += dk_new
            parts.append(dot(k_t[head * HEAD_DIM:(head + 1) * HEAD_DIM, :], ds_t))
        z = jnp.concatenate(parts, axis=0).T
        z = (z * cos[cols, :] - swap_halves(z) * sin[cols, :]) * HEAD_DIM ** -0.5
        dq_sum = dq_sum + col_sum(z)
        dq_out[cols, :] = z.astype(BF16)
    z = dk_acc[...]
    z = z * cos[...] - swap_halves(z) * sin[...]
    dk_out[...] = z.astype(BF16)
    z_v = dv_acc[...]
    dv_out[...] = z_v.astype(BF16)
    sums[0] = jnp.concatenate([dq_sum, col_sum(z), col_sum(z_v)], axis=0)


FF_CHUNK = 768


def ffn_kernel(ctx, x_in, grad_y, w_out, w_fc1, w_fc2, vec,
               y_out, dmid_out, dctx_out, gw_out, gw_fc1, gw_fc2, g_small, g_b1, y_acc, dh_acc):
    step = pl.program_id(0)
    @pl.when(step == 0)
    def _():
        for ref in (gw_out, gw_fc1, gw_fc2, g_small, g_b1):
            ref[...] = jnp.zeros_like(ref)

    gain, b_fc1 = vec_row(vec, 'ln2_gain'), vec_row(vec, 'b_fc1')
    ctx_val = ctx[...]
    x_mid = x_in[...].astype(F32) + dot(ctx_val, w_out[...]) + vec_row(vec, 'b_out')
    x_hat, inv_std = hat_of(x_mid)
    h_two = (x_hat * gain + vec_row(vec, 'ln2_bias')).astype(BF16)
    dy = grad_y[...]
    y_acc[...] = x_mid + vec_row(vec, 'b_fc2')
    for j in range(w_fc1.shape[1] // FF_CHUNK):
        cols = slice(j * FF_CHUNK, (j + 1) * FF_CHUNK)
        pre = dot(h_two, w_fc1[:, cols]) + b_fc1[:, cols]
        cdf = 0.5 + 0.5 * lax.erf(pre * (0.5 ** 0.5))
        pdf = jnp.exp(pre * pre * -0.5) * 0.3989422804014327
        act = (pre * cdf).astype(BF16)
        d_act = dot(dy, w_fc2[cols, :], NT)
        d_pre = d_act * (cdf + pre * pdf)
        y_acc[...] += dot(act, w_fc2[cols, :])
        gw_fc2[cols, :] += dot(act, dy, TN)
        g_b1[:, cols] += col_sum(d_pre)
        d_pre = d_pre.astype(BF16)
        gw_fc1[j] += dot(h_two, d_pre, TN)
        d_h = dot(d_pre, w_fc1[:, cols], NT)
        if j == 0:
            dh_acc[...] = d_h
        else:
            dh_acc[...] += d_h
    y_out[...] = y_acc[...].astype(BF16)
    d_two = dh_acc[...]
    dy_f = dy.astype(F32)
    d_mid = dy_f + hat_bwd(d_two, x_hat, inv_std, gain)
    dmid_out[...] = d_mid
    for row, grad in enumerate((d_mid, d_two * x_hat, d_two, dy_f)):
        g_small[row:row + 1, :] += col_sum(grad)
    d_mid = d_mid.astype(BF16)
    gw_out[...] += dot(ctx_val, d_mid, TN)
    dctx_out[...] = dot(d_mid, w_out[...], NT).astype(BF16)


def whole(shape):
    return pl.BlockSpec(shape, lambda *_: (0,) * len(shape), pipeline_mode=pl.Buffered(1))


def shape_of(dims, dtype):
    return jax.ShapeDtypeStruct(dims, dtype)


def call(kernel, grid, in_specs, out_specs, out_shape, args, flops, scratch=(), name=None, collective_id=None):
    moved = sum(a.size * a.dtype.itemsize for a in args) + sum(o.size * o.dtype.itemsize for o in out_shape)
    return pl.pallas_call(
        kernel, grid=grid, in_specs=in_specs, out_specs=out_specs, out_shape=out_shape,
        scratch_shapes=list(scratch), name=name,
        compiler_params=pltpu.CompilerParams(vmem_limit_bytes=VMEM_LIMIT,
                                             dimension_semantics=('arbitrary',) * len(grid),
                                             collective_id=collective_id,
                                             has_side_effects=collective_id is not None),
        cost_estimate=pl.CostEstimate(flops=flops, bytes_accessed=moved, transcendentals=0))(*args)


def layer_compute(tokens, grad_y, vec_part, weights):
    seqs, seq_len = tokens.shape
    dim, ff = grad_y.shape[2], weights[2].shape[1]
    n_tok, pairs, half = seqs * seq_len, dim // PAIR, dim // 2
    cos, sin = rope_tables(seq_len)
    tok_seq = tokens.reshape(seqs, 1, seq_len)
    any_spec = pl.BlockSpec(memory_space=pl.ANY)
    wide = shape_of((n_tok, dim), BF16)
    wide_f32 = shape_of((n_tok, dim), F32)

    def rows_spec(rows, width=dim):
        return pl.BlockSpec((rows, width), lambda i: (i, 0))

    def wholes(*arrays):
        return [whole(a.shape) for a in arrays]

    def sems(*counts):
        return [pltpu.SemaphoreType.DMA((n,)) for n in counts]

    tile = 256
    per_seq = seq_len // tile
    table_spec = pl.BlockSpec((tile, PAIR), lambda i: (i % per_seq, 0))
    full = [shape_of((2 * w.shape[0],) + w.shape[1:], BF16) for w in weights]
    vec_shape = shape_of((2,) + vec_part.shape, BF16)
    x_in, q, k, v, vec, w_qkv, w_out, w_fc1, w_fc2 = call(
        qkv_kernel, (n_tok // tile,),
        [pl.BlockSpec((1, 1, seq_len), lambda i: (i // per_seq, 0, 0)),
         pl.BlockSpec((1, 1, tile), lambda i: (i, 0, 0)), any_spec, table_spec, table_spec] + [any_spec] * 4,
        [rows_spec(tile)] * 4 + wholes(vec_shape) + [any_spec] * 4, [wide] * 4 + [vec_shape] + full,
        (tok_seq, tokens.reshape(n_tok // tile, 1, tile), vec_part, cos, sin) + tuple(weights),
        6 * n_tok * dim * dim,
        scratch=[pltpu.VMEM(full[0].shape, BF16), pltpu.VMEM(vec_shape.shape, BF16)]
        + [pltpu.VMEM(w.shape, BF16) for w in weights[1:]] + sems(5, 5, 9), name='qkv', collective_id=2)

    head_spec = pl.BlockSpec((seq_len, PAIR), lambda b, p: (b, p))
    tok_spec = pl.BlockSpec((1, 1, seq_len), lambda b, p: (b, 0, 0))
    lse_spec = pl.BlockSpec((1, 2, seq_len), lambda b, p: (b * pairs + p, 0, 0))
    ctx, lse = call(
        attn_fwd_kernel, (seqs, pairs), [head_spec] * 3 + [tok_spec], [head_spec, lse_spec],
        [wide, shape_of((seqs * pairs, 2, seq_len), F32)],
        (q, k, v, tok_seq), 16 * n_tok * seq_len * dim, name='attn_fwd')

    tile = 512
    pages = shape_of((ff // dim, dim, dim), F32)
    grads = [shape_of(w_out.shape, F32), pages, shape_of(w_fc2.shape, F32), shape_of((8, dim), F32),
             shape_of((1, ff), F32)]
    hidden, d_mid, d_ctx, gw_out, gw_fc1, gw_fc2, small_two, g_b1 = call(
        ffn_kernel, (n_tok // tile,), [rows_spec(tile)] * 3 + wholes(w_out, w_fc1, w_fc2, vec),
        [rows_spec(tile)] * 3 + wholes(*grads), [wide, wide_f32, wide] + grads,
        (ctx, x_in, grad_y.reshape(n_tok, dim), w_out, w_fc1, w_fc2, vec),
        6 * n_tok * dim * (dim + 2 * ff), scratch=[pltpu.VMEM((tile, dim), F32)] * 2, name='ffn')

    blocks = (3, RING, RING, half // (3 * RING * RING), dim)
    whole_table = pl.BlockSpec((seq_len, PAIR), lambda b, p: (0, 0))
    red_shape = shape_of((3, 2) + blocks[3:], F32)
    sum_shape = shape_of((seqs * pairs, 3, PAIR), F32)
    n_sems = 2 + 6 * FLOW_SEMS
    dq, dk, dv, b_sums, red = call(
        attn_bwd_reduce_kernel, (seqs, pairs),
        [head_spec] * 4 + [lse_spec, tok_spec, whole_table, whole_table, any_spec, any_spec],
        [head_spec] * 3 + [pl.BlockSpec((1, 3, PAIR), lambda b, p: (b * pairs + p, 0, 0))] + wholes(red_shape),
        [wide] * 3 + [sum_shape, red_shape],
        (q, k, v, d_ctx, lse, tok_seq, cos, sin, gw_fc2.reshape((2, RING) + blocks), gw_fc1.reshape((RING, 2) + blocks)),
        40 * n_tok * seq_len * dim,
        scratch=[pltpu.VMEM((seq_len, PAIR), F32)] * 2 + [pltpu.VMEM((RING, 2) + blocks, F32)] * 2
        + comm_temps(2, blocks[3], dim) + sems(n_sems, n_sems, 2), name='attn_bwd', collective_id=0)

    n_sems = 16 + 12 * FLOW_SEMS
    fc2, fc1, out, qkv, small_sum = call(
        qkv_bwd_reduce_kernel, (seqs,),
        [pl.BlockSpec((1, 1, seq_len), lambda i: (i, 0, 0))] + [rows_spec(seq_len)] * 5
        + wholes(w_qkv, vec, red, small_two, g_b1, b_sums) + [any_spec],
        [any_spec] * 4 + [whole((SMALL_ROWS, half))],
        [shape_of((RING,) + blocks, F32), shape_of(blocks[:-1] + (ff,), F32), shape_of(blocks, F32),
         shape_of(blocks[:-1] + (3 * dim,), F32), shape_of((SMALL_ROWS, half), F32)],
        (tok_seq, x_in, dq, dk, dv, d_mid, w_qkv, vec, red, small_two, g_b1, b_sums, gw_out.reshape((2,) + blocks)),
        12 * n_tok * dim * dim,
        scratch=[pltpu.VMEM((RING, 2) + blocks, F32), pltpu.VMEM((RING, 1) + blocks, F32)]
        + comm_temps(1, blocks[3], dim)
        + [pltpu.VMEM((RING, 2) + blocks, F32), pltpu.VMEM((2, SMALL_ROWS, half), F32),
           pltpu.VMEM((SMALL_ROWS, half), F32), pltpu.VMEM((3, RING, SMALL_ROWS, half), F32)]
        + sems(n_sems, n_sems, 10), name='qkv_bwd', collective_id=1)
    big = (qkv.reshape(half, 3 * dim), out.reshape(half, dim), fc1.reshape(half, ff), fc2.reshape(ff // 2, dim))
    return hidden.reshape(grad_y.shape), big, small_sum


RING = 4
ALL = slice(None)
ORDERS = ('xyz', 'yzx', 'zxy')
STRIDE = {'x': 1, 'y': RING, 'z': RING * RING}
MESH_ID = pl.DeviceIdType.MESH


class Torus:
    def __init__(self):
        self.me = lax.axis_index('dp')
        self.part = lax.axis_index('fsdp')
        self.coord = {axis: self.me // stride % RING for axis, stride in STRIDE.items()}

    def at(self, axis, delta):
        return (self.coord[axis] + delta + RING) % RING

    def chip(self, axis, delta):
        return {'dp': self.me + (self.at(axis, delta) - self.coord[axis]) * STRIDE[axis]}

    def partner(self):
        return {'fsdp': 1 - self.part}

    def greet(self):
        barrier = pltpu.get_barrier_semaphore()
        peers = [self.partner()] + [self.chip(axis, delta) for axis in 'xyz' for delta in (1, -1)]
        for peer in peers:
            pl.semaphore_signal(barrier, inc=1, device_id=peer, device_id_type=MESH_ID)
        pl.semaphore_wait(barrier, len(peers))


class Flow:
    def __init__(self, torus, order, sign, view, temp_view, grads, sums, temps, sends, recvs, base):
        self.torus, self.order, self.sign = torus, order, sign
        self.view, self.temp_view = view, temp_view
        self.grads, self.sums, self.temps = grads, sums, temps
        self.sends, self.recvs, self.base = sends, recvs, base
        self.used = []

    def route(self, slot):
        level, kind = slot % 9 // 3, slot % 3
        sign = self.sign
        if slot < 9:
            target = self.temp_view(self.temps, level, kind)
            if kind == 2:
                return self.temp_view(self.temps, level, 0), target, level, sign
            delta = (2, -sign)[kind]
            return self.view(self.grads, self.place(level, delta)), target, level, (sign, -sign)[kind]
        if kind == 2:
            block = self.view(self.sums, self.place(level, -sign))
            return block, block, level, sign
        target = self.view(self.sums, self.place(level + 1))
        source = self.final(self) if level == 2 else target
        return source, target, level, (sign, -sign)[kind]

    def copy(self, slot):
        src, dst, level, delta = self.route(slot)
        return pltpu.make_async_remote_copy(
            src_ref=src, dst_ref=dst, send_sem=self.sends.at[self.base + slot],
            recv_sem=self.recvs.at[self.base + slot],
            device_id=self.torus.chip(self.order[level], delta), device_id_type=MESH_ID)

    def start(self, slot):
        self.used.append(slot)
        self.copy(slot).start()

    def wait(self, slot):
        self.copy(slot).wait_recv()

    def place(self, level, delta=None):
        own = [self.torus.coord[axis] for axis in self.order[:level]]
        return tuple(own) + (() if delta is None else (self.torus.at(self.order[level], delta),))

    def scatter_start(self, level):
        self.start(level * 3)
        self.start(level * 3 + 1)

    def scatter_mid(self, level):
        self.wait(level * 3)
        relay = self.temp_view(self.temps, level, 0)
        relay[...] = relay[...] + self.view(self.grads, self.place(level, self.sign))[...]
        self.start(level * 3 + 2)

    def scatter_end(self, level):
        self.wait(level * 3 + 1)
        self.wait(level * 3 + 2)
        mine = self.view(self.grads, self.place(level, 0))
        mine[...] = mine[...] + self.temp_view(self.temps, level, 1)[...] + self.temp_view(self.temps, level, 2)[...]

    def gather_start(self, level):
        if level == 2:
            self.view(self.sums, self.place(3))[...] = self.final(self)[...]
        self.start(9 + level * 3)
        self.start(10 + level * 3)

    def gather_mid(self, level):
        self.wait(9 + level * 3)
        self.start(11 + level * 3)

    def gather_end(self, level):
        self.wait(10 + level * 3)
        self.wait(11 + level * 3)

    def scatter_next(self, level):
        self.scatter_end(level)
        if level == 2:
            self.gather_start(level)
        else:
            self.scatter_start(level + 1)

    def gather_next(self, level):
        self.gather_end(level)
        self.gather_start(level - 1)

    def finish(self):
        for slot in self.used:
            self.copy(slot).wait_send()


FLOW_SEMS = 18


def own_block(flow):
    return flow.view(flow.grads, flow.place(3))


def make_flows(torus, width, grads, sums, temps, sends, recvs, base, group=ALL, final=own_block):
    half = width // 2
    flows = []
    for color, order in enumerate(ORDERS):
        for side, sign in enumerate((1, -1)):
            lanes = pl.ds(side * half, half)

            def view(ref, place, color=color, lanes=lanes):
                rest = place[1:] + (ALL,) * (4 - len(place))
                return ref.at[(place[0], group if ref is grads else ALL, color) + rest + (lanes,)]

            def temp_view(refs, level, kind, color=color, lanes=lanes):
                return refs[level].at[(kind, ALL, color) + (ALL,) * (3 - level) + (lanes,)]

            flow = Flow(torus, order, sign, view, temp_view, grads, sums, temps, sends, recvs,
                        base + len(flows) * FLOW_SEMS)
            flow.final, flow.color, flow.lanes = final, color, lanes
            flows.append(flow)
    return flows


def each(flows, name, level):
    for flow in flows:
        getattr(flow, name)(level)


def comm_temps(groups, rows, dim):
    return [pltpu.VMEM((3, groups, 3) + (RING,) * (2 - level) + (rows, dim), F32) for level in range(3)]


def attn_bwd_reduce_kernel(q, k, v, d_ctx, lse, tok_seq, cos, sin, fc2, fc1, dq_out, dk_out, dv_out, sums_out, red,
                           dk_acc, dv_acc, grads, other_sum, temp0, temp1, temp2, sends, recvs, local):
    torus = Torus()
    step = pl.program_id(0) * pl.num_programs(1) + pl.program_id(1)
    flows = make_flows(torus, grads.shape[-1], grads, None, (temp0, temp1, temp2), sends, recvs, 2)
    sources = (lambda i: fc2.at[i], lambda i: fc1.at[:, i])

    def remote(n):
        return pltpu.make_async_remote_copy(
            src_ref=sources[n](1 - torus.part), dst_ref=other_sum.at[:, n], send_sem=sends.at[n], recv_sem=recvs.at[n],
            device_id=torus.partner(), device_id_type=MESH_ID)

    def mine(n):
        return pltpu.make_async_copy(sources[n](torus.part), grads.at[:, n], local.at[n])

    @pl.when(step == 0)
    def _():
        torus.greet()
        for n in range(2):
            remote(n).start()
            mine(n).start()

    @pl.when(step == 4)
    def _():
        for n in range(2):
            remote(n).wait_recv()
            mine(n).wait()

            @pl.loop(0, RING * 3)
            def _(i):
                grads[i // 3, n, i % 3] = grads[i // 3, n, i % 3] + other_sum[i // 3, n, i % 3]
        each(flows, 'scatter_start', 0)

    @pl.when(step == 8)
    def _():
        each(flows, 'scatter_mid', 0)

    @pl.when(step == 10)
    def _():
        each(flows, 'scatter_next', 0)

    @pl.when(step == 11)
    def _():
        each(flows, 'scatter_mid', 1)

    attn_bwd_kernel(q, k, v, d_ctx, lse, tok_seq, cos, sin, dq_out, dk_out, dv_out, sums_out, dk_acc, dv_acc)

    @pl.when(step == 11)
    def _():
        each(flows, 'scatter_next', 1)
        each(flows, 'scatter_mid', 2)
        each(flows, 'scatter_end', 2)
        for flow in flows:
            red[flow.color, :, :, flow.lanes] = own_block(flow)[...]
        for n in range(2):
            remote(n).wait_send()
        for flow in flows:
            flow.finish()


def qkv_bwd_reduce_kernel(tok_seq, x_in, dq, dk, dv, d_mid, w_qkv, vec, red, small_two, g_b1, b_sums,
                          gw_out, fc2_sum, fc1_sum, out_sum, qkv_sum, small_sum,
                          grads, sums, temp0, temp1, temp2, sums_ab, small, small_other, small_slots,
                          sends, recvs, local):
    torus = Torus()
    step = pl.program_id(0)
    last = pl.num_programs(0) - 1
    dim = x_in.shape[1]
    half = dim // 2
    part = torus.part

    def final(flow):
        return red.at[flow.color, :, :, flow.lanes]

    gathers = make_flows(torus, dim, None, sums_ab, None, sends, recvs, 16, final=final)
    flows = make_flows(torus, dim, grads, sums, (temp0, temp1, temp2), sends, recvs, 16 + 6 * FLOW_SEMS,
                       group=pl.ds(part, 1))

    def load_out():
        return pltpu.make_async_copy(gw_out, grads.at[0], local.at[0])

    def later_hook():
        each(gathers, 'gather_next', 2)
        each(gathers, 'gather_mid', 1)

    hooks = ((0, 1, lambda: each(gathers, 'gather_mid', 2)), (0, 2, later_hook), (1, 0, lambda: each(gathers, 'gather_next', 1)))

    @pl.when(step == 0)
    def _():
        torus.greet()
        load_out().start()
        each(gathers, 'gather_start', 2)
        small[...] = jnp.zeros_like(small)
        for page in range(1, RING):
            grads[page] = jnp.zeros(grads.shape[1:], F32)

    x_hat, inv_std = hat_of(x_in[...].astype(F32))
    gain = vec_row(vec, 'ln1_gain')
    h_one = (x_hat * gain + vec_row(vec, 'ln1_bias')).astype(BF16)
    d_one = None
    for index, ref in enumerate((dq, dk, dv)):
        for at_step, at_index, hook in hooks:
            if at_index == index:
                pl.when(step == at_step)(hook)
        cols = slice(index * dim, (index + 1) * dim)
        d_part = ref[...]
        grads[index + 1] += dot(h_one, d_part, TN).reshape(grads.shape[1:])
        new = dot(d_part, w_qkv[:, cols], NT)
        d_one = new if index == 0 else d_one + new
    g_rows = jnp.concatenate([col_sum(d_one * x_hat), col_sum(d_one)], axis=0)
    d_in = d_mid[...] + hat_bwd(d_one, x_hat, inv_std, gain)
    scale, _ = seq_counts(tok_seq[0])
    one_hot = live_one_hot(tok_seq[0], EMB_ROWS)
    high = d_in.astype(BF16)
    low = (d_in - high.astype(F32)).astype(BF16)
    g_emb = (dot(one_hot, high) + dot(one_hot, low)) * scale
    for side in range(2):
        lanes = slice(side * half, (side + 1) * half)
        small[side, :EMB_ROWS, :] += g_emb[:, lanes]
        small[side, EMB_ROWS:EMB_ROWS + 2, :] += g_rows[:, lanes]

    @pl.when(step == last)
    def _():
        load_out().wait()
        pairs = dim // 128
        per_pair = [b_sums[p] for p in range(pairs)]
        for b in range(1, b_sums.shape[0] // pairs):
            per_pair = [per_pair[p] + b_sums[b * pairs + p] for p in range(pairs)]
        b_qkv = jnp.concatenate([per_pair[p][i:i + 1] for i in range(3) for p in range(pairs)], axis=1)
        for side in range(2):
            row = EMB_ROWS + 2
            small[side, row:row + 4, :] = small_two[:4, side * half:(side + 1) * half]
            row += 4
            for grad in (b_qkv, g_b1[...]):
                base = side * (grad.shape[1] // 2)
                for i in range(grad.shape[1] // dim):
                    small[side, row:row + 1, :] = grad[:, base + i * half:base + (i + 1) * half]
                    row += 1
        pair_copies = [
            pltpu.make_async_remote_copy(
                src_ref=small.at[1 - part], dst_ref=small_other, send_sem=sends.at[0], recv_sem=recvs.at[0],
                device_id=torus.partner(), device_id_type=MESH_ID)] + [
            pltpu.make_async_remote_copy(
                src_ref=grads.at[page, 1 - part], dst_ref=sums.at[page, 0], send_sem=sends.at[1 + page],
                recv_sem=recvs.at[1 + page], device_id=torus.partner(), device_id_type=MESH_ID)
            for page in range(RING)]
        for copy in pair_copies:
            copy.start()
        started = list(pair_copies)

        def small_start(level, value):
            axis = ORDERS[0][level]
            here = torus.coord[axis]
            small_slots[level, here] = value
            slot = small_slots.at[level, here]
            copies = [pltpu.make_async_remote_copy(
                src_ref=slot, dst_ref=slot, send_sem=sends.at[5 + level * 3 + n], recv_sem=recvs.at[5 + level * 3 + n],
                device_id=torus.chip(axis, delta), device_id_type=MESH_ID) for n, delta in enumerate((1, -1, 2))]
            for copy in copies:
                copy.start()
            started.extend(copies)
            return copies

        def small_end(level, copies):
            for copy in copies:
                copy.wait_recv()
            return ((small_slots[level, 0] + small_slots[level, 1]) + small_slots[level, 2]) + small_slots[level, 3]

        pair_copies[0].wait_recv()
        small_copies = small_start(0, small[part] + small_other[...])
        for page in range(RING):
            pair_copies[1 + page].wait_recv()

            @pl.loop(0, 3)
            def _(i):
                grads[page, part, i] = grads[page, part, i] + sums[page, 0, i]
        each(flows, 'scatter_start', 0)
        each(gathers, 'gather_mid', 0)
        for level in range(3):
            each(flows, 'scatter_mid', level)
            total = small_end(level, small_copies)
            if level < 2:
                small_copies = small_start(level + 1, total)
            each(flows, 'scatter_next', level)
        small_sum[...] = total
        each(gathers, 'gather_end', 0)
        stores = [pltpu.make_async_copy(sums_ab.at[:, 0], fc2_sum, local.at[1])]
        for page in range(RING):
            lanes = pl.ds(page * dim, dim)
            stores.append(pltpu.make_async_copy(sums_ab.at[page, 1], fc1_sum.at[:, :, :, :, lanes], local.at[2 + page]))
        for store in stores:
            store.start()
        each(flows, 'gather_mid', 2)
        for level in (1, 0):
            each(flows, 'gather_next', level + 1)
            each(flows, 'gather_mid', level)
        each(flows, 'gather_end', 0)
        tail = [pltpu.make_async_copy(sums.at[0, 0], out_sum, local.at[6])]
        for page in range(3):
            tail.append(pltpu.make_async_copy(
                sums.at[page + 1, 0], qkv_sum.at[:, :, :, :, pl.ds(page * dim, dim)], local.at[7 + page]))
        for store in tail:
            store.start()
        for copy in started:
            copy.wait_send()
        for flow in gathers + flows:
            flow.finish()
        for store in stores + tail:
            store.wait()


def solution(mesh):
    row_spec = P(('dp', 'fsdp'), None)
    act_spec = P(('dp', 'fsdp'), None, None)
    param_specs = (P(None, 'fsdp'),) + (P('fsdp'),) * 12

    def local_step(tokens, grad_y, *shards):
        (embedding, ln1_gain, ln1_bias, w_qkv, b_qkv, w_out, b_out,
         ln2_gain, ln2_bias, w_fc1, b_fc1, w_fc2, b_fc2) = shards
        vectors = (ln1_gain, ln1_bias, b_out, ln2_gain, ln2_bias, b_fc2, b_qkv, b_fc1)
        vocab, width = embedding.shape
        rows = [vec.reshape(-1, width) for vec in vectors]
        vec_part = jnp.concatenate([jnp.pad(embedding, ((0, VEC_ROW - vocab), (0, 0)))] + rows)
        vec_part = jnp.pad(vec_part, ((0, SMALL_ROWS - vec_part.shape[0]), (0, 0)))
        hidden, big, small_sum = layer_compute(tokens, grad_y, vec_part, (w_qkv, w_out, w_fc1, w_fc2))
        g_w_qkv, g_w_out, g_w_fc1, g_w_fc2 = big
        g_embedding = small_sum[:vocab]
        start = EMB_ROWS
        vec_grads = []
        for row in rows:
            vec_grads.append(small_sum[start:start + row.shape[0]].reshape(-1))
            start += row.shape[0]
        (g_ln1_gain, g_ln1_bias, g_b_out, g_ln2_gain, g_ln2_bias, g_b_fc2, g_b_qkv, g_b_fc1) = vec_grads
        return (hidden, g_embedding, g_ln1_gain, g_ln1_bias, g_w_qkv, g_b_qkv, g_w_out, g_b_out,
                g_ln2_gain, g_ln2_bias, g_w_fc1, g_b_fc1, g_w_fc2, g_b_fc2)

    return jax.shard_map(local_step, mesh=mesh, in_specs=(row_spec, act_spec) + param_specs,
                         out_specs=(act_spec,) + param_specs, check_vma=False)
```

```python
import functools
import jax
import jax.numpy as jnp
import numpy as np
from jax import lax
from jax.experimental import pallas as pl
from jax.experimental.pallas import tpu as pltpu
from jax.sharding import PartitionSpec as P

HEAD_DIM = 64
MASK_ID = 32
PAD_ID = 1
MASK_RATIO = 0.15 * 0.8
LN_EPS = 1e-5
ROPE_BASE = 10000.0
F32 = jnp.float32
BF16 = jnp.bfloat16
EMB_ROWS = 40
SMALL_ROWS = 64
VEC_ROW = 48
VECTORS = ('ln1_gain', 'ln1_bias', 'b_out', 'ln2_gain', 'ln2_bias', 'b_fc2', 'b_qkv', 'b_fc1')
SCALE = HEAD_DIM ** -0.5
VMEM_LIMIT = 60 << 20

NN = (((1,), (0,)), ((), ()))
NT = (((1,), (1,)), ((), ()))
TN = (((0,), (0,)), ((), ()))


def dot(lhs, rhs, dims=NN):
    return lax.dot_general(lhs, rhs, dims, preferred_element_type=F32)


def row_mean(x_val):
    return jnp.mean(x_val, axis=-1, keepdims=True)


def hat_of(x_val):
    centered = x_val - row_mean(x_val)
    inv_std = lax.rsqrt(row_mean(centered * centered) + LN_EPS)
    return centered * inv_std, inv_std


def hat_bwd(d_out, x_hat, inv_std, gain):
    d_hat = d_out * gain
    return inv_std * (d_hat - row_mean(d_hat)
                      - x_hat * row_mean(d_hat * x_hat))


def rope_tables(seq_len):
    power = np.arange(0, HEAD_DIM, 2, dtype=np.float32) / np.float32(HEAD_DIM)
    inv_freq = np.float32(1) / np.power(np.float32(ROPE_BASE), power)
    angles = np.outer(np.arange(seq_len, dtype=np.float32), inv_freq).astype(np.float64)
    cos, sin = np.cos(angles), np.sin(angles)
    return (jnp.asarray(np.concatenate([cos] * 4, axis=1), F32),
            jnp.asarray(np.concatenate([-sin, sin] * 2, axis=1), F32))


def col_sum(x_val):
    return jnp.sum(x_val, axis=0, keepdims=True)


def iota(shape, dim):
    return lax.broadcasted_iota(jnp.int32, shape, dim)


def vec_row(vec, name):
    at = VECTORS.index(name)
    count = {'b_qkv': 3, 'b_fc1': 4}.get(name, 1)
    row = VEC_ROW + at + (2 if name == 'b_fc1' else 0)
    return jnp.concatenate([vec[side, i:i + 1, :] for side in range(2) for i in range(row, row + count)],
                           axis=1).astype(F32)


def seq_counts(tok_row):
    masks = jnp.sum((tok_row == MASK_ID).astype(F32), axis=1, keepdims=True)
    real = jnp.sum((tok_row != PAD_ID).astype(F32), axis=1, keepdims=True)
    return (1.0 - MASK_RATIO) / (1.0 - masks / real), real


def live_one_hot(tok_row, rows):
    live = (tok_row == iota((rows, tok_row.shape[1]), 0)) & (tok_row != MASK_ID) & (tok_row != PAD_ID)
    return live.astype(F32).astype(BF16)


def swap_halves(x_val):
    low = (iota(x_val.shape, 1) & 32) == 0
    return jnp.where(low, pltpu.roll(x_val, 96, 1), pltpu.roll(x_val, 32, 1))


def rows_of_head(x_val, head):
    return jnp.where((iota(x_val.shape, 0) >= HEAD_DIM) == (head == 1), x_val, jnp.zeros_like(x_val))


def lanes_of_head(x_val, head):
    return jnp.where((iota(x_val.shape, 1) >= HEAD_DIM) == (head == 1), x_val, jnp.zeros_like(x_val))


def qkv_kernel(tok_seq, vec_part, cos, sin, wq_part, wo_part, w1_part, w2_part,
               x_out, q_out, k_out, v_out, vec_out, wq_out, wo_out, w1_out, w2_out,
               w_qkv, vec, wo_own, w1_own, w2_own, sends, recvs, local):
    step = pl.program_id(0)
    part = lax.axis_index('fsdp')
    partner = {'fsdp': 1 - part}
    dim = x_out.shape[1]

    def own_rows(ref):
        size = ref.shape[0] // 2
        return ref.at[pl.ds(part * size, size)]

    moves = [(wq_part, w_qkv), (vec_part, vec.at[part]), (wo_own, wo_out), (w1_own, w1_out), (w2_own, w2_out)]

    def target(n):
        return moves[n][1] if n == 1 else own_rows(moves[n][1])

    def remote(n):
        return pltpu.make_async_remote_copy(
            src_ref=moves[n][0], dst_ref=target(n), send_sem=sends.at[n], recv_sem=recvs.at[n],
            device_id=partner, device_id_type=MESH_ID)

    def keep_own(n):
        return pltpu.make_async_copy(moves[n][0], target(n), local.at[n])

    stage = ((wo_part, wo_own), (w1_part, w1_own), (w2_part, w2_own))

    def store_qkv():
        return pltpu.make_async_copy(w_qkv, wq_out, local.at[len(moves) + len(stage)])

    @pl.when(step == 0)
    def _():
        barrier = pltpu.get_barrier_semaphore()
        pl.semaphore_signal(barrier, inc=1, device_id=partner, device_id_type=MESH_ID)
        pl.semaphore_wait(barrier, 1)
        for n in range(2):
            remote(n).start()
            keep_own(n).start()
        loads = [pltpu.make_async_copy(src, dst, local.at[len(moves) + n]) for n, (src, dst) in enumerate(stage)]
        for copy in loads:
            copy.start()
        for n, copy in enumerate(loads):
            copy.wait()
            remote(n + 2).start()
            keep_own(n + 2).start()
        for n in range(2):
            remote(n).wait_recv()
            keep_own(n).wait()
        store_qkv().start()
        vec_out[...] = vec[...]

    per_seq = tok_seq.shape[2] // x_out.shape[0]
    first = lax.rem(step, per_seq) * x_out.shape[0]
    tok_tile = tok_seq[0, :, pl.ds(pl.multiple_of(first, x_out.shape[0]), x_out.shape[0])]
    scale, _ = seq_counts(tok_seq[0])
    emb = jnp.concatenate([vec[side, :VEC_ROW, :] for side in range(2)], axis=1)
    x_b16 = (dot(live_one_hot(tok_tile, VEC_ROW), emb, TN) * scale).astype(BF16)
    x_out[...] = x_b16
    x_hat, _ = hat_of(x_b16.astype(F32))
    h_one = (x_hat * vec_row(vec, 'ln1_gain') + vec_row(vec, 'ln1_bias')).astype(BF16)
    cos_tab, sin_tab = cos[...], sin[...]
    b_qkv = vec_row(vec, 'b_qkv')
    for index, out in enumerate((q_out, k_out, v_out)):
        cols = slice(index * dim, (index + 1) * dim)
        proj = dot(h_one, w_qkv[:, cols]) + b_qkv[:, cols]
        if out is v_out:
            out[...] = proj.astype(BF16)
            continue
        if out is q_out:
            proj = proj * SCALE
        for first in range(0, dim, PAIR):
            pair = slice(first, first + PAIR)
            z = proj[:, pair]
            out[:, pair] = (z * cos_tab + swap_halves(z) * sin_tab).astype(BF16)

    @pl.when(step == pl.num_programs(0) - 1)
    def _():
        store_qkv().wait()
        for n in range(len(moves)):
            remote(n).wait_send()
            if n >= 2:
                remote(n).wait_recv()
                keep_own(n).wait()


PAIR = 2 * HEAD_DIM
def pad_bias(tok_row):
    _, real = seq_counts(tok_row)
    size = tok_row.shape[1]
    return jnp.where(iota((size, size), 0).astype(F32) < real, 0.0, -1e30)


def head_rows(head):
    return slice(head * HEAD_DIM, (head + 1) * HEAD_DIM)


def attn_fwd_kernel(q, k, v, tok_seq, ctx, lse):
    q_t, v_t, k_val = q[...].T, v[...].T, k[...]
    bias = pad_bias(tok_seq[0])
    parts = []
    for head in range(2):
        s_t = dot(k_val, rows_of_head(q_t, head)) + bias
        top = jnp.max(s_t, axis=0, keepdims=True)
        e_t = jnp.exp(s_t - top)
        total = col_sum(e_t)
        lse[0, head:head + 1, :] = top + jnp.log(total)
        p_t = (e_t * (1.0 / total)).astype(BF16)
        parts.append(dot(v_t[head_rows(head), :], p_t))
    ctx[...] = jnp.concatenate(parts, axis=0).T.astype(BF16)


def attn_bwd_kernel(q, k, v, d_ctx, lse, tok_seq, cos, sin, dq_out, dk_out, dv_out, sums):
    q_val, k_val, v_val, d_val = q[...], k[...], v[...], d_ctx[...]
    q_t, k_t, d_t = q_val.T, k_val.T, d_val.T
    bias = pad_bias(tok_seq[0])
    parts, d_key, d_value = [], 0.0, 0.0
    for head in range(2):
        s_t = dot(k_val, rows_of_head(q_t, head)) + bias
        p_t = jnp.exp(s_t - lse[0, head:head + 1, :])
        dp_t = dot(v_val, rows_of_head(d_t, head))
        delta = col_sum(p_t * dp_t)
        ds_t = (p_t * (dp_t - delta)).astype(BF16)
        d_value += dot(p_t.astype(BF16), lanes_of_head(d_val, head))
        d_key += dot(ds_t, lanes_of_head(q_val, head))
        parts.append(dot(k_t[head_rows(head), :], ds_t))

    def unrotate(z):
        return z * cos[...] - swap_halves(z) * sin[...]

    grads = (unrotate(jnp.concatenate(parts, axis=0).T) * SCALE, unrotate(d_key), d_value)
    for grad, out in zip(grads, (dq_out, dk_out, dv_out)):
        out[...] = grad.astype(BF16)
    sums[0] = jnp.concatenate([col_sum(grad) for grad in grads], axis=0)


FF_CHUNK = 768


def ffn_kernel(ctx, x_in, grad_y, wo_hbm, w1_hbm, w2_hbm, vec,
               y_out, dmid_out, dctx_out, gwo_hbm, gw1_hbm, gw2_hbm, g_small, g_b1,
               y_acc, dh_acc, w_out, w_fc1, w_fc2, gw_out, gw_fc1, gw_fc2, b_fc1, local):
    step = pl.program_id(0)
    chunks = w_fc1.shape[1] // FF_CHUNK

    def cols(j):
        return pl.ds(j * FF_CHUNK, FF_CHUNK)

    def loads(j):
        if j == chunks:
            return [pltpu.make_async_copy(wo_hbm, w_out, local.at[2 * j])]
        return [pltpu.make_async_copy(w1_hbm.at[:, cols(j)], w_fc1.at[:, cols(j)], local.at[2 * j]),
                pltpu.make_async_copy(w2_hbm.at[cols(j)], w_fc2.at[cols(j)], local.at[2 * j + 1])]

    def stores(j):
        if j == chunks:
            return [pltpu.make_async_copy(gw_out, gwo_hbm, local.at[2 * j])]
        return [pltpu.make_async_copy(gw_fc1.at[j], gw1_hbm.at[j], local.at[2 * j]),
                pltpu.make_async_copy(gw_fc2.at[cols(j)], gw2_hbm.at[cols(j)], local.at[2 * j + 1])]

    def at_first(j):
        @pl.when(step == 0)
        def _():
            for copy in loads(j):
                copy.wait()

    def at_last(j):
        @pl.when(step == pl.num_programs(0) - 1)
        def _():
            for copy in stores(j):
                copy.start()

    @pl.when(step == 0)
    def _():
        for j in [chunks] + list(range(chunks)):
            for copy in loads(j):
                copy.start()
        for ref in (gw_out, gw_fc1, gw_fc2, g_small, g_b1):
            ref[...] = jnp.zeros_like(ref)
        b_fc1[...] = vec_row(vec, 'b_fc1')

    gain = vec_row(vec, 'ln2_gain')
    ctx_val = ctx[...]
    at_first(chunks)
    x_mid = x_in[...].astype(F32) + dot(ctx_val, w_out[...]) + vec_row(vec, 'b_out')
    x_hat, inv_std = hat_of(x_mid)
    h_two = (x_hat * gain + vec_row(vec, 'ln2_bias')).astype(BF16)
    dy = grad_y[...]
    y_acc[...] = x_mid + vec_row(vec, 'b_fc2')
    dh_acc[...] = jnp.zeros_like(dh_acc)
    for j in range(chunks):
        at_first(j)
        pre = dot(h_two, w_fc1[:, cols(j)]) + b_fc1[:, cols(j)]
        cdf = 0.5 + 0.5 * lax.erf(pre * (0.5 ** 0.5))
        pdf = jnp.exp(pre * pre * -0.5) * 0.3989422804014327
        act = (pre * cdf).astype(BF16)
        d_act = dot(dy, w_fc2[cols(j), :], NT)
        d_pre = d_act * (cdf + pre * pdf)
        y_acc[...] += dot(act, w_fc2[cols(j), :])
        gw_fc2[cols(j), :] += dot(act, dy, TN)
        g_b1[:, cols(j)] += col_sum(d_pre)
        d_pre = d_pre.astype(BF16)
        gw_fc1[j] += dot(h_two, d_pre, TN)
        dh_acc[...] += dot(d_pre, w_fc1[:, cols(j)], NT)
        if j > 0:
            at_last(j - 1)
    at_last(chunks - 1)
    y_out[...] = y_acc[...].astype(BF16)
    d_two = dh_acc[...]
    dy_f = dy.astype(F32)
    d_mid = dy_f + hat_bwd(d_two, x_hat, inv_std, gain)
    dmid_out[...] = d_mid
    for row, grad in enumerate((d_mid, d_two * x_hat, d_two, dy_f)):
        g_small[row:row + 1, :] += col_sum(grad)
    d_mid = d_mid.astype(BF16)
    gw_out[...] += dot(ctx_val, d_mid, TN)
    dctx_out[...] = dot(d_mid, w_out[...], NT).astype(BF16)
    at_last(chunks)

    @pl.when(step == pl.num_programs(0) - 1)
    def _():
        for j in range(chunks + 1):
            for copy in stores(j):
                copy.wait()


def whole(shape):
    return pl.BlockSpec(shape, lambda *_: (0,) * len(shape), pipeline_mode=pl.Buffered(1))


def shape_of(dims, dtype):
    return jax.ShapeDtypeStruct(dims, dtype)


def call(kernel, grid, in_specs, out_specs, out_shape, args, flops, scratch=(), name=None, collective_id=None):
    moved = sum(a.size * a.dtype.itemsize for a in args) + sum(o.size * o.dtype.itemsize for o in out_shape)
    return pl.pallas_call(
        kernel, grid=grid, in_specs=in_specs, out_specs=out_specs, out_shape=out_shape,
        scratch_shapes=list(scratch), name=name,
        compiler_params=pltpu.CompilerParams(vmem_limit_bytes=VMEM_LIMIT,
                                             dimension_semantics=('arbitrary',) * len(grid),
                                             collective_id=collective_id,
                                             has_side_effects=collective_id is not None),
        cost_estimate=pl.CostEstimate(flops=flops, bytes_accessed=moved, transcendentals=0))(*args)


def layer_compute(tokens, grad_y, vec_part, weights):
    seqs, seq_len = tokens.shape
    dim, ff = grad_y.shape[2], weights[2].shape[1]
    n_tok, pairs, half = seqs * seq_len, dim // PAIR, dim // 2
    cos, sin = rope_tables(seq_len)
    tok_seq = tokens.reshape(seqs, 1, seq_len)
    any_spec = pl.BlockSpec(memory_space=pl.ANY)
    wide = shape_of((n_tok, dim), BF16)
    wide_f32 = shape_of((n_tok, dim), F32)

    def rows_spec(rows, width=dim):
        return pl.BlockSpec((rows, width), lambda i: (i, 0))

    def wholes(*arrays):
        return [whole(a.shape) for a in arrays]

    def sems(*counts):
        return [pltpu.SemaphoreType.DMA((n,)) for n in counts]

    tile = 256
    per_seq = seq_len // tile
    table_spec = pl.BlockSpec((tile, PAIR), lambda i: (i % per_seq, 0))
    full = [shape_of((2 * w.shape[0],) + w.shape[1:], BF16) for w in weights]
    vec_shape = shape_of((2,) + vec_part.shape, BF16)
    x_in, q, k, v, vec, w_qkv, w_out, w_fc1, w_fc2 = call(
        qkv_kernel, (n_tok // tile,),
        [pl.BlockSpec((1, 1, seq_len), lambda i: (i // per_seq, 0, 0)),
         any_spec, table_spec, table_spec] + [any_spec] * 4,
        [rows_spec(tile)] * 4 + wholes(vec_shape) + [any_spec] * 4, [wide] * 4 + [vec_shape] + full,
        (tok_seq, vec_part, cos, sin) + tuple(weights),
        6 * n_tok * dim * dim,
        scratch=[pltpu.VMEM(full[0].shape, BF16), pltpu.VMEM(vec_shape.shape, BF16)]
        + [pltpu.VMEM(w.shape, BF16) for w in weights[1:]] + sems(5, 5, 9), name='qkv', collective_id=2)

    head_spec = pl.BlockSpec((seq_len, PAIR), lambda b, p: (b, p))
    tok_spec = pl.BlockSpec((1, 1, seq_len), lambda b, p: (b, 0, 0))
    lse_spec = pl.BlockSpec((1, 2, seq_len), lambda b, p: (b * pairs + p, 0, 0))
    ctx, lse = call(
        attn_fwd_kernel, (seqs, pairs), [head_spec] * 3 + [tok_spec], [head_spec, lse_spec],
        [wide, shape_of((seqs * pairs, 2, seq_len), F32)],
        (q, k, v, tok_seq), 16 * n_tok * seq_len * dim, name='attn_fwd')

    tile = 512
    pages = shape_of((ff // dim, dim, dim), F32)
    grads = [shape_of(w_out.shape, F32), pages, shape_of(w_fc2.shape, F32), shape_of((8, dim), F32),
             shape_of((1, ff), F32)]
    hidden, d_mid, d_ctx, gw_out, gw_fc1, gw_fc2, small_two, g_b1 = call(
        ffn_kernel, (n_tok // tile,), [rows_spec(tile)] * 3 + [any_spec] * 3 + wholes(vec),
        [rows_spec(tile)] * 3 + [any_spec] * 3 + wholes(*grads[3:]), [wide, wide_f32, wide] + grads,
        (ctx, x_in, grad_y.reshape(n_tok, dim), w_out, w_fc1, w_fc2, vec),
        6 * n_tok * dim * (dim + 2 * ff), scratch=[pltpu.VMEM((tile, dim), F32)] * 2 + [pltpu.VMEM(w.shape, BF16) for w in (w_out, w_fc1, w_fc2)]
        + [pltpu.VMEM(g.shape, F32) for g in grads[:3]] + [pltpu.VMEM((1, ff), F32)] + sems(2 * ff // dim + 1), name='ffn')

    blocks = (3, RING, RING, half // (3 * RING * RING), dim)
    whole_table = pl.BlockSpec((seq_len, PAIR), lambda b, p: (0, 0))
    red_shape = shape_of((3, 2) + blocks[3:], F32)
    sum_shape = shape_of((seqs * pairs, 3, PAIR), F32)
    n_sems = 2 + 12 * SCATTER_SEMS
    dq, dk, dv, b_sums, red = call(
        attn_bwd_reduce_kernel, (seqs, pairs),
        [head_spec] * 4 + [lse_spec, tok_spec, whole_table, whole_table, any_spec, any_spec],
        [head_spec] * 3 + [pl.BlockSpec((1, 3, PAIR), lambda b, p: (b * pairs + p, 0, 0))] + wholes(red_shape),
        [wide] * 3 + [sum_shape, red_shape],
        (q, k, v, d_ctx, lse, tok_seq, cos, sin, gw_fc2.reshape((2, RING) + blocks), gw_fc1.reshape((RING, 2) + blocks)),
        40 * n_tok * seq_len * dim,
        scratch=[pltpu.VMEM((RING, 2) + blocks, F32)] * 2
        + comm_temps(2, blocks[3], dim) + sems(n_sems, n_sems, 2), name='attn_bwd', collective_id=0)

    n_sems = 16 + 12 * FLOW_SEMS
    fc2, fc1, out, qkv, small_sum = call(
        qkv_bwd_reduce_kernel, (seqs,),
        [pl.BlockSpec((1, 1, seq_len), lambda i: (i, 0, 0))] + [rows_spec(seq_len)] * 5
        + wholes(w_qkv, vec, red, small_two, g_b1, b_sums) + [any_spec],
        [any_spec] * 4 + [whole((SMALL_ROWS, half))],
        [shape_of((RING,) + blocks, F32), shape_of(blocks[:-1] + (ff,), F32), shape_of(blocks, F32),
         shape_of(blocks[:-1] + (3 * dim,), F32), shape_of((SMALL_ROWS, half), F32)],
        (tok_seq, x_in, dq, dk, dv, d_mid, w_qkv, vec, red, small_two, g_b1, b_sums, gw_out.reshape((2,) + blocks)),
        12 * n_tok * dim * dim,
        scratch=[pltpu.VMEM((RING, 2) + blocks, F32), pltpu.VMEM((RING, 1) + blocks, F32)]
        + comm_temps(1, blocks[3], dim)
        + [pltpu.VMEM((RING, 2) + blocks, F32), pltpu.VMEM((2, SMALL_ROWS, half), F32),
           pltpu.VMEM((SMALL_ROWS, half), F32), pltpu.VMEM((3, RING, SMALL_ROWS, half), F32)]
        + sems(n_sems, n_sems, 10), name='qkv_bwd', collective_id=1)
    big = (qkv.reshape(half, 3 * dim), out.reshape(half, dim), fc1.reshape(half, ff), fc2.reshape(ff // 2, dim))
    return hidden.reshape(grad_y.shape), big, small_sum


RING = 4
ALL = slice(None)
ORDERS = ('xyz', 'yzx', 'zxy')
STRIDE = {'x': 1, 'y': RING, 'z': RING * RING}
MESH_ID = pl.DeviceIdType.MESH


class Torus:
    def __init__(self):
        self.me = lax.axis_index('dp')
        self.part = lax.axis_index('fsdp')
        self.coord = {axis: self.me // stride % RING for axis, stride in STRIDE.items()}

    def at(self, axis, delta):
        return (self.coord[axis] + delta + RING) % RING

    def chip(self, axis, delta):
        return {'dp': self.me + (self.at(axis, delta) - self.coord[axis]) * STRIDE[axis]}

    def partner(self):
        return {'fsdp': 1 - self.part}

    def greet(self):
        barrier = pltpu.get_barrier_semaphore()
        peers = [self.partner()] + [self.chip(axis, delta) for axis in 'xyz' for delta in (1, -1)]
        for peer in peers:
            pl.semaphore_signal(barrier, inc=1, device_id=peer, device_id_type=MESH_ID)
        pl.semaphore_wait(barrier, len(peers))


class Flow:
    def __init__(self, torus, order, sign, view, temp_view, grads, sums, temps, sends, recvs, base):
        self.torus, self.order, self.sign = torus, order, sign
        self.view, self.temp_view = view, temp_view
        self.grads, self.sums, self.temps = grads, sums, temps
        self.sends, self.recvs, self.base = sends, recvs, base
        self.used = []

    def route(self, slot):
        level, kind = slot % 9 // 3, slot % 3
        sign = self.sign
        if slot < 9:
            target = self.temp_view(self.temps, level, kind)
            if kind == 2:
                return self.temp_view(self.temps, level, 0), target, level, sign
            delta = (2, -sign)[kind]
            return self.view(self.grads, self.place(level, delta)), target, level, (sign, -sign)[kind]
        if kind == 2:
            block = self.view(self.sums, self.place(level, -sign))
            return block, block, level, sign
        target = self.view(self.sums, self.place(level + 1))
        source = self.final(self) if level == 2 else target
        return source, target, level, (sign, -sign)[kind]

    def copy(self, slot):
        src, dst, level, delta = self.route(slot)
        return pltpu.make_async_remote_copy(
            src_ref=src, dst_ref=dst, send_sem=self.sends.at[self.base + slot],
            recv_sem=self.recvs.at[self.base + slot],
            device_id=self.torus.chip(self.order[level], delta), device_id_type=MESH_ID)

    def start(self, slot):
        self.used.append(slot)
        self.copy(slot).start()

    def wait(self, slot):
        self.copy(slot).wait_recv()

    def place(self, level, delta=None):
        own = [self.torus.coord[axis] for axis in self.order[:level]]
        return tuple(own) + (() if delta is None else (self.torus.at(self.order[level], delta),))

    def scatter_start(self, level):
        self.start(level * 3)
        self.start(level * 3 + 1)

    def scatter_mid(self, level):
        self.wait(level * 3)
        relay = self.temp_view(self.temps, level, 0)
        relay[...] = relay[...] + self.view(self.grads, self.place(level, self.sign))[...]
        self.start(level * 3 + 2)

    def scatter_end(self, level):
        self.wait(level * 3 + 1)
        self.wait(level * 3 + 2)
        mine = self.view(self.grads, self.place(level, 0))
        mine[...] = mine[...] + self.temp_view(self.temps, level, 1)[...] + self.temp_view(self.temps, level, 2)[...]

    def gather_start(self, level):
        if level == 2:
            self.view(self.sums, self.place(3))[...] = self.final(self)[...]
        self.start(9 + level * 3)
        self.start(10 + level * 3)

    def gather_mid(self, level):
        self.wait(9 + level * 3)
        self.start(11 + level * 3)

    def gather_end(self, level):
        self.wait(10 + level * 3)
        self.wait(11 + level * 3)

    def scatter_next(self, level):
        self.scatter_end(level)
        if level == 2:
            self.gather_start(level)
        else:
            self.scatter_start(level + 1)

    def gather_next(self, level):
        self.gather_end(level)
        self.gather_start(level - 1)

    def finish(self):
        for slot in self.used:
            self.copy(slot).wait_send()


FLOW_SEMS = 18
SCATTER_SEMS = 9


def own_block(flow):
    return flow.view(flow.grads, flow.place(3))


def make_flows(torus, width, grads, sums, temps, sends, recvs, base, group=ALL, temp_group=ALL, final=own_block,
               spacing=FLOW_SEMS):
    half = width // 2
    flows = []
    for color, order in enumerate(ORDERS):
        for side, sign in enumerate((1, -1)):
            lanes = pl.ds(side * half, half)

            def view(ref, place, color=color, lanes=lanes):
                rest = place[1:] + (ALL,) * (4 - len(place))
                return ref.at[(place[0], group if ref is grads else ALL, color) + rest + (lanes,)]

            def temp_view(refs, level, kind, color=color, lanes=lanes):
                return refs[level].at[(kind, temp_group, color) + (ALL,) * (3 - level) + (lanes,)]

            flow = Flow(torus, order, sign, view, temp_view, grads, sums, temps, sends, recvs,
                        base + len(flows) * spacing)
            flow.final, flow.color, flow.lanes = final, color, lanes
            flows.append(flow)
    return flows


def each(flows, name, level):
    for flow in flows:
        getattr(flow, name)(level)


def comm_temps(groups, rows, dim):
    return [pltpu.VMEM((3, groups, 3) + (RING,) * (2 - level) + (rows, dim), F32) for level in range(3)]


PLAN = ('b', '', 'e0', '', '', 'm00 e1', '', 'a00', 'm01 m10', 'a01', 'm02 a10', 'm11 a02', 'a11 m12 a12')


def attn_bwd_reduce_kernel(q, k, v, d_ctx, lse, tok_seq, cos, sin, fc2, fc1, dq_out, dk_out, dv_out, sums_out, red,
                           grads, other_sum, temp0, temp1, temp2, sends, recvs, local):
    torus = Torus()
    step = pl.program_id(0) * pl.num_programs(1) + pl.program_id(1)
    sets = [make_flows(torus, grads.shape[-1], grads, None, (temp0, temp1, temp2), sends, recvs,
                       2 + n * 6 * SCATTER_SEMS, group=pl.ds(n, 1), temp_group=pl.ds(n, 1), spacing=SCATTER_SEMS)
            for n in range(2)]
    sources = (lambda i: fc2.at[i], lambda i: fc1.at[:, i])

    def remote(n):
        return pltpu.make_async_remote_copy(
            src_ref=sources[n](1 - torus.part), dst_ref=other_sum.at[:, n], send_sem=sends.at[n], recv_sem=recvs.at[n],
            device_id=torus.partner(), device_id_type=MESH_ID)

    def mine(n):
        return pltpu.make_async_copy(sources[n](torus.part), grads.at[:, n], local.at[n])

    def begin():
        torus.greet()
        for n in range(2):
            remote(n).start()
            mine(n).start()

    def enter(n):
        remote(n).wait_recv()
        mine(n).wait()

        @pl.loop(0, RING)
        def _(page):
            grads[page, n] = grads[page, n] + other_sum[page, n]
        each(sets[n], 'scatter_start', 0)

    def mid(n, level):
        each(sets[n], 'scatter_mid', level)

    def after(n, level):
        each(sets[n], 'scatter_next' if level < 2 else 'scatter_end', level)

    actions = {'b': begin, 'e': enter, 'm': mid, 'a': after}

    def perform(words):
        for word in words.split():
            actions[word[0]](*(int(number) for number in word[1:]))

    for at_step, words in enumerate(PLAN[:-1]):
        pl.when(step == at_step)(functools.partial(perform, words))

    attn_bwd_kernel(q, k, v, d_ctx, lse, tok_seq, cos, sin, dq_out, dk_out, dv_out, sums_out)

    @pl.when(step == len(PLAN) - 2)
    def _():
        perform(PLAN[-1])
        for n, flows in enumerate(sets):
            for flow in flows:
                red[flow.color, n:n + 1, :, flow.lanes] = own_block(flow)[...]
                flow.finish()
            remote(n).wait_send()


def qkv_bwd_reduce_kernel(tok_seq, x_in, dq, dk, dv, d_mid, w_qkv, vec, red, small_two, g_b1, b_sums,
                          gw_out, fc2_sum, fc1_sum, out_sum, qkv_sum, small_sum,
                          grads, sums, temp0, temp1, temp2, sums_ab, small, small_other, small_slots,
                          sends, recvs, local):
    torus = Torus()
    step = pl.program_id(0)
    last = pl.num_programs(0) - 1
    dim = x_in.shape[1]
    half = dim // 2
    part = torus.part

    def final(flow):
        return red.at[flow.color, :, :, flow.lanes]

    gathers = make_flows(torus, dim, None, sums_ab, None, sends, recvs, 16, final=final)
    flows = make_flows(torus, dim, grads, sums, (temp0, temp1, temp2), sends, recvs, 16 + 6 * FLOW_SEMS,
                       group=pl.ds(part, 1))

    def load_out():
        return pltpu.make_async_copy(gw_out, grads.at[0], local.at[0])

    def later_hook():
        each(gathers, 'gather_next', 2)
        each(gathers, 'gather_mid', 1)

    def last_hook():
        each(gathers, 'gather_next', 1)
        load_out().wait()

    hooks = ((0, 1, lambda: each(gathers, 'gather_mid', 2)), (0, 2, later_hook), (1, 0, last_hook))

    def pair_copy(page):
        return pltpu.make_async_remote_copy(
            src_ref=grads.at[page, 1 - part], dst_ref=sums.at[page, 0], send_sem=sends.at[1 + page],
            recv_sem=recvs.at[1 + page], device_id=torus.partner(), device_id_type=MESH_ID)

    @pl.when(step == 0)
    def _():
        torus.greet()
        load_out().start()
        each(gathers, 'gather_start', 2)
        small[...] = jnp.zeros_like(small)
        for page in range(1, RING):
            grads[page] = jnp.zeros(grads.shape[1:], F32)

    x_hat, inv_std = hat_of(x_in[...].astype(F32))
    gain = vec_row(vec, 'ln1_gain')
    h_one = (x_hat * gain + vec_row(vec, 'ln1_bias')).astype(BF16)
    d_one = None
    for index, ref in enumerate((dq, dk, dv)):
        for at_step, at_index, hook in hooks:
            if at_index == index:
                pl.when(step == at_step)(hook)
        cols = slice(index * dim, (index + 1) * dim)
        d_part = ref[...]
        grads[index + 1] += dot(h_one, d_part, TN).reshape(grads.shape[1:])
        new = dot(d_part, w_qkv[:, cols], NT)
        pl.when(step == last)(pair_copy(index).start)
        d_one = new if index == 0 else d_one + new
    g_rows = jnp.concatenate([col_sum(d_one * x_hat), col_sum(d_one)], axis=0)
    d_in = d_mid[...] + hat_bwd(d_one, x_hat, inv_std, gain)
    scale, _ = seq_counts(tok_seq[0])
    one_hot = live_one_hot(tok_seq[0], EMB_ROWS)
    high = d_in.astype(BF16)
    low = (d_in - high.astype(F32)).astype(BF16)
    g_emb = (dot(one_hot, high) + dot(one_hot, low)) * scale
    for side in range(2):
        lanes = slice(side * half, (side + 1) * half)
        small[side, :EMB_ROWS, :] += g_emb[:, lanes]
        small[side, EMB_ROWS:EMB_ROWS + 2, :] += g_rows[:, lanes]

    @pl.when(step == last)
    def _():
        pair_copy(RING - 1).start()
        pairs = dim // PAIR
        per_pair = [b_sums[p] for p in range(pairs)]
        for b in range(1, b_sums.shape[0] // pairs):
            per_pair = [per_pair[p] + b_sums[b * pairs + p] for p in range(pairs)]
        b_qkv = jnp.concatenate([per_pair[p][i:i + 1] for i in range(3) for p in range(pairs)], axis=1)
        for side in range(2):
            row = EMB_ROWS + 2
            small[side, row:row + 4, :] = small_two[:4, side * half:(side + 1) * half]
            row += 4
            for grad in (b_qkv, g_b1[...]):
                base = side * (grad.shape[1] // 2)
                for i in range(grad.shape[1] // dim):
                    small[side, row:row + 1, :] = grad[:, base + i * half:base + (i + 1) * half]
                    row += 1
        small_copy = pltpu.make_async_remote_copy(
            src_ref=small.at[1 - part], dst_ref=small_other, send_sem=sends.at[0], recv_sem=recvs.at[0],
            device_id=torus.partner(), device_id_type=MESH_ID)
        small_copy.start()
        started = [small_copy] + [pair_copy(page) for page in range(RING)]

        def small_start(level, value):
            axis = ORDERS[0][level]
            here = torus.coord[axis]
            small_slots[level, here] = value
            slot = small_slots.at[level, here]
            copies = [pltpu.make_async_remote_copy(
                src_ref=slot, dst_ref=slot, send_sem=sends.at[5 + level * 3 + n], recv_sem=recvs.at[5 + level * 3 + n],
                device_id=torus.chip(axis, delta), device_id_type=MESH_ID) for n, delta in enumerate((1, -1, 2))]
            for copy in copies:
                copy.start()
            started.extend(copies)
            return copies

        def small_end(level, copies):
            for copy in copies:
                copy.wait_recv()
            return ((small_slots[level, 0] + small_slots[level, 1]) + small_slots[level, 2]) + small_slots[level, 3]

        small_copy.wait_recv()
        small_copies = small_start(0, small[part] + small_other[...])
        for page in range(RING):
            started[1 + page].wait_recv()

            @pl.loop(0, 3)
            def _(i):
                grads[page, part, i] = grads[page, part, i] + sums[page, 0, i]
        each(flows, 'scatter_start', 0)
        each(gathers, 'gather_mid', 0)
        for level in range(3):
            each(flows, 'scatter_mid', level)
            total = small_end(level, small_copies)
            if level < 2:
                small_copies = small_start(level + 1, total)
            each(flows, 'scatter_next', level)
        small_sum[...] = total
        each(gathers, 'gather_end', 0)
        stores = [pltpu.make_async_copy(sums_ab.at[:, 0], fc2_sum, local.at[1])]
        for page in range(RING):
            lanes = pl.ds(page * dim, dim)
            stores.append(pltpu.make_async_copy(sums_ab.at[page, 1], fc1_sum.at[:, :, :, :, lanes], local.at[2 + page]))
        for store in stores:
            store.start()
        each(flows, 'gather_mid', 2)
        for level in (1, 0):
            each(flows, 'gather_next', level + 1)
            each(flows, 'gather_mid', level)
        each(flows, 'gather_end', 0)
        tail = [pltpu.make_async_copy(sums.at[0, 0], out_sum, local.at[6])]
        for page in range(3):
            tail.append(pltpu.make_async_copy(
                sums.at[page + 1, 0], qkv_sum.at[:, :, :, :, pl.ds(page * dim, dim)], local.at[7 + page]))
        for store in tail:
            store.start()
        for copy in started:
            copy.wait_send()
        for flow in gathers + flows:
            flow.finish()
        for store in stores + tail:
            store.wait()


def solution(mesh):
    row_spec = P(('dp', 'fsdp'), None)
    act_spec = P(('dp', 'fsdp'), None, None)
    param_specs = (P(None, 'fsdp'),) + (P('fsdp'),) * 12

    def local_step(tokens, grad_y, *shards):
        (embedding, ln1_gain, ln1_bias, w_qkv, b_qkv, w_out, b_out,
         ln2_gain, ln2_bias, w_fc1, b_fc1, w_fc2, b_fc2) = shards
        vectors = (ln1_gain, ln1_bias, b_out, ln2_gain, ln2_bias, b_fc2, b_qkv, b_fc1)
        vocab, width = embedding.shape
        flat = jnp.concatenate(vectors)
        vec_part = jnp.concatenate([jnp.pad(embedding, ((0, VEC_ROW - vocab), (0, 0))), flat.reshape(-1, width)])
        vec_part = jnp.pad(vec_part, ((0, SMALL_ROWS - vec_part.shape[0]), (0, 0)))
        hidden, big, small_sum = layer_compute(tokens, grad_y, vec_part, (w_qkv, w_out, w_fc1, w_fc2))
        g_w_qkv, g_w_out, g_w_fc1, g_w_fc2 = big
        g_embedding = small_sum[:vocab]
        start = EMB_ROWS
        vec_grads = []
        for vec in vectors:
            stop = start + vec.size // width
            vec_grads.append(small_sum[start:stop].reshape(-1))
            start = stop
        (g_ln1_gain, g_ln1_bias, g_b_out, g_ln2_gain, g_ln2_bias, g_b_fc2, g_b_qkv, g_b_fc1) = vec_grads
        return (hidden, g_embedding, g_ln1_gain, g_ln1_bias, g_w_qkv, g_b_qkv, g_w_out, g_b_out,
                g_ln2_gain, g_ln2_bias, g_w_fc1, g_b_fc1, g_w_fc2, g_b_fc2)

    return jax.shard_map(local_step, mesh=mesh, in_specs=(row_spec, act_spec) + param_specs,
                         out_specs=(act_spec,) + param_specs, check_vma=False)
```

```python
import functools
import jax
import jax.numpy as jnp
import numpy as np
from jax import lax
from jax.experimental import pallas as pl
from jax.experimental.pallas import tpu as pltpu
from jax.sharding import PartitionSpec as P

HEAD_DIM = 64
MASK_ID = 32
PAD_ID = 1
MASK_RATIO = 0.15 * 0.8
LN_EPS = 1e-5
ROPE_BASE = 10000.0
F32 = jnp.float32
BF16 = jnp.bfloat16
EMB_ROWS = 40
SMALL_ROWS = 64
VEC_ROW = 48
VECTORS = ('ln1_gain', 'ln1_bias', 'b_out', 'ln2_gain', 'ln2_bias', 'b_fc2', 'b_qkv', 'b_fc1')
SCALE = HEAD_DIM ** -0.5
VMEM_LIMIT = 60 << 20

NN = (((1,), (0,)), ((), ()))
NT = (((1,), (1,)), ((), ()))
TN = (((0,), (0,)), ((), ()))


def dot(lhs, rhs, dims=NN):
    return lax.dot_general(lhs, rhs, dims, preferred_element_type=F32)


def row_mean(x_val):
    return jnp.mean(x_val, axis=-1, keepdims=True)


def hat_of(x_val):
    centered = x_val - row_mean(x_val)
    inv_std = lax.rsqrt(row_mean(centered * centered) + LN_EPS)
    return centered * inv_std, inv_std


def hat_bwd(d_out, x_hat, inv_std, gain):
    d_hat = d_out * gain
    return inv_std * (d_hat - row_mean(d_hat)
                      - x_hat * row_mean(d_hat * x_hat))


def rope_tables(seq_len):
    power = np.arange(0, HEAD_DIM, 2, dtype=np.float32) / np.float32(HEAD_DIM)
    inv_freq = np.float32(1) / np.power(np.float32(ROPE_BASE), power)
    angles = np.outer(np.arange(seq_len, dtype=np.float32), inv_freq).astype(np.float64)
    cos, sin = np.cos(angles), np.sin(angles)
    return (jnp.asarray(np.concatenate([cos] * 4, axis=1), F32),
            jnp.asarray(np.concatenate([-sin, sin] * 2, axis=1), F32))


def col_sum(x_val):
    return jnp.sum(x_val, axis=0, keepdims=True)


def iota(shape, dim):
    return lax.broadcasted_iota(jnp.int32, shape, dim)


def vec_row(vec, name):
    at = VECTORS.index(name)
    count = {'b_qkv': 3, 'b_fc1': 4}.get(name, 1)
    row = VEC_ROW + at + (2 if name == 'b_fc1' else 0)
    return jnp.concatenate([vec[side, i:i + 1, :] for side in range(2) for i in range(row, row + count)],
                           axis=1).astype(F32)


def seq_counts(tok_row):
    masks = jnp.sum((tok_row == MASK_ID).astype(F32), axis=1, keepdims=True)
    real = jnp.sum((tok_row != PAD_ID).astype(F32), axis=1, keepdims=True)
    return (1.0 - MASK_RATIO) / (1.0 - masks / real), real


def live_one_hot(tok_row, rows):
    live = (tok_row == iota((rows, tok_row.shape[1]), 0)) & (tok_row != MASK_ID) & (tok_row != PAD_ID)
    return live.astype(F32).astype(BF16)


def swap_halves(x_val):
    low = (iota(x_val.shape, 1) & 32) == 0
    return jnp.where(low, pltpu.roll(x_val, 96, 1), pltpu.roll(x_val, 32, 1))


def rows_of_head(x_val, head):
    return jnp.where((iota(x_val.shape, 0) >= HEAD_DIM) == (head == 1), x_val, jnp.zeros_like(x_val))


def lanes_of_head(x_val, head):
    return jnp.where((iota(x_val.shape, 1) >= HEAD_DIM) == (head == 1), x_val, jnp.zeros_like(x_val))


def qkv_kernel(tok_seq, vec_part, cos, sin, wq_part, wo_part, w1_part, w2_part,
               x_out, q_out, k_out, v_out, vec_out, wq_out, wo_out, w1_out, w2_out,
               w_qkv, vec, wo_own, w1_own, w2_own, sends, recvs, local):
    step = pl.program_id(0)
    part = lax.axis_index('fsdp')
    partner = {'fsdp': 1 - part}
    dim = x_out.shape[1]

    def own_rows(ref):
        size = ref.shape[0] // 2
        return ref.at[pl.ds(part * size, size)]

    moves = [(wq_part, w_qkv), (vec_part, vec.at[part]), (wo_own, wo_out), (w1_own, w1_out), (w2_own, w2_out)]

    def target(n):
        return moves[n][1] if n == 1 else own_rows(moves[n][1])

    def remote(n):
        return pltpu.make_async_remote_copy(
            src_ref=moves[n][0], dst_ref=target(n), send_sem=sends.at[n], recv_sem=recvs.at[n],
            device_id=partner, device_id_type=MESH_ID)

    def keep_own(n):
        return pltpu.make_async_copy(moves[n][0], target(n), local.at[n])

    stage = ((wo_part, wo_own), (w1_part, w1_own), (w2_part, w2_own))

    def store_qkv():
        return pltpu.make_async_copy(w_qkv, wq_out, local.at[len(moves) + len(stage)])

    @pl.when(step == 0)
    def _():
        barrier = pltpu.get_barrier_semaphore()
        pl.semaphore_signal(barrier, inc=1, device_id=partner, device_id_type=MESH_ID)
        pl.semaphore_wait(barrier, 1)
        for n in range(2):
            remote(n).start()
            keep_own(n).start()
        loads = [pltpu.make_async_copy(src, dst, local.at[len(moves) + n]) for n, (src, dst) in enumerate(stage)]
        for copy in loads:
            copy.start()
        for n, copy in enumerate(loads):
            copy.wait()
            remote(n + 2).start()
            keep_own(n + 2).start()
        for n in range(2):
            remote(n).wait_recv()
            keep_own(n).wait()
        store_qkv().start()
        vec_out[...] = vec[...]

    per_seq = tok_seq.shape[2] // x_out.shape[0]
    first = lax.rem(step, per_seq) * x_out.shape[0]
    tok_tile = tok_seq[0, :, pl.ds(pl.multiple_of(first, x_out.shape[0]), x_out.shape[0])]
    scale, _ = seq_counts(tok_seq[0])
    emb = jnp.concatenate([vec[side, :VEC_ROW, :] for side in range(2)], axis=1)
    x_b16 = (dot(live_one_hot(tok_tile, VEC_ROW), emb, TN) * scale).astype(BF16)
    x_out[...] = x_b16
    x_hat, _ = hat_of(x_b16.astype(F32))
    h_one = (x_hat * vec_row(vec, 'ln1_gain') + vec_row(vec, 'ln1_bias')).astype(BF16)
    cos_tab, sin_tab = cos[...], sin[...]
    b_qkv = vec_row(vec, 'b_qkv')
    for index, out in enumerate((q_out, k_out, v_out)):
        cols = slice(index * dim, (index + 1) * dim)
        proj = dot(h_one, w_qkv[:, cols]) + b_qkv[:, cols]
        if out is v_out:
            out[...] = proj.astype(BF16)
            continue
        if out is q_out:
            proj = proj * SCALE
        for first in range(0, dim, PAIR):
            pair = slice(first, first + PAIR)
            z = proj[:, pair]
            out[:, pair] = (z * cos_tab + swap_halves(z) * sin_tab).astype(BF16)

    @pl.when(step == pl.num_programs(0) - 1)
    def _():
        store_qkv().wait()
        for n in range(len(moves)):
            remote(n).wait_send()
            if n >= 2:
                remote(n).wait_recv()
                keep_own(n).wait()


PAIR = 2 * HEAD_DIM
def pad_bias(tok_row):
    _, real = seq_counts(tok_row)
    size = tok_row.shape[1]
    return jnp.where(iota((size, size), 0).astype(F32) < real, 0.0, -1e30)


def head_rows(head):
    return slice(head * HEAD_DIM, (head + 1) * HEAD_DIM)


def attn_fwd_kernel(q, k, v, tok_seq, ctx, lse):
    q_t, v_t, k_val = q[...].T, v[...].T, k[...]
    bias = pad_bias(tok_seq[0])
    parts = []
    for head in range(2):
        s_t = dot(k_val, rows_of_head(q_t, head)) + bias
        top = jnp.max(s_t, axis=0, keepdims=True)
        e_t = jnp.exp(s_t - top)
        total = col_sum(e_t)
        lse[0, head:head + 1, :] = top + jnp.log(total)
        p_t = (e_t * (1.0 / total)).astype(BF16)
        parts.append(dot(v_t[head_rows(head), :], p_t))
    ctx[...] = jnp.concatenate(parts, axis=0).T.astype(BF16)


def attn_bwd_kernel(q, k, v, d_ctx, lse, tok_seq, cos, sin, dq_out, dk_out, dv_out, sums):
    q_val, k_val, v_val, d_val = q[...], k[...], v[...], d_ctx[...]
    q_t, k_t, d_t = q_val.T, k_val.T, d_val.T
    bias = pad_bias(tok_seq[0])
    parts, d_key, d_value = [], 0.0, 0.0
    for head in range(2):
        s_t = dot(k_val, rows_of_head(q_t, head)) + bias
        p_t = jnp.exp(s_t - lse[0, head:head + 1, :])
        dp_t = dot(v_val, rows_of_head(d_t, head))
        delta = col_sum(p_t * dp_t)
        ds_t = (p_t * (dp_t - delta)).astype(BF16)
        d_value += dot(p_t.astype(BF16), lanes_of_head(d_val, head))
        d_key += dot(ds_t, lanes_of_head(q_val, head))
        parts.append(dot(k_t[head_rows(head), :], ds_t))

    def unrotate(z):
        return z * cos[...] - swap_halves(z) * sin[...]

    grads = (unrotate(jnp.concatenate(parts, axis=0).T) * SCALE, unrotate(d_key), d_value)
    for grad, out in zip(grads, (dq_out, dk_out, dv_out)):
        out[...] = grad.astype(BF16)
    sums[0] = jnp.concatenate([col_sum(grad) for grad in grads], axis=0)


FF_CHUNK = 768


def ffn_kernel(ctx, x_in, grad_y, wo_hbm, w1_hbm, w2_hbm, vec,
               y_out, dmid_out, dctx_out, gwo_hbm, gw1_hbm, gw2_hbm, g_small, g_b1,
               y_acc, dh_acc, w_out, w_fc1, w_fc2, gw_out, gw_fc1, gw_fc2, b_fc1, local):
    step = pl.program_id(0)
    chunks = w_fc1.shape[1] // FF_CHUNK

    def cols(j):
        return pl.ds(j * FF_CHUNK, FF_CHUNK)

    def loads(j):
        if j == chunks:
            return [pltpu.make_async_copy(wo_hbm, w_out, local.at[2 * j])]
        return [pltpu.make_async_copy(w1_hbm.at[:, cols(j)], w_fc1.at[:, cols(j)], local.at[2 * j]),
                pltpu.make_async_copy(w2_hbm.at[cols(j)], w_fc2.at[cols(j)], local.at[2 * j + 1])]

    def stores(j):
        if j == chunks:
            return [pltpu.make_async_copy(gw_out, gwo_hbm, local.at[2 * j])]
        return [pltpu.make_async_copy(gw_fc1.at[j], gw1_hbm.at[j], local.at[2 * j]),
                pltpu.make_async_copy(gw_fc2.at[cols(j)], gw2_hbm.at[cols(j)], local.at[2 * j + 1])]

    def at_first(j):
        @pl.when(step == 0)
        def _():
            for copy in loads(j):
                copy.wait()

    def at_last(j):
        @pl.when(step == pl.num_programs(0) - 1)
        def _():
            for copy in stores(j):
                copy.start()

    @pl.when(step == 0)
    def _():
        for j in [chunks] + list(range(chunks)):
            for copy in loads(j):
                copy.start()
        for ref in (gw_out, gw_fc1, gw_fc2, g_small, g_b1):
            ref[...] = jnp.zeros_like(ref)
        b_fc1[...] = vec_row(vec, 'b_fc1')

    gain = vec_row(vec, 'ln2_gain')
    ctx_val = ctx[...]
    at_first(chunks)
    x_mid = x_in[...].astype(F32) + dot(ctx_val, w_out[...]) + vec_row(vec, 'b_out')
    x_hat, inv_std = hat_of(x_mid)
    h_two = (x_hat * gain + vec_row(vec, 'ln2_bias')).astype(BF16)
    dy = grad_y[...]
    y_acc[...] = x_mid + vec_row(vec, 'b_fc2')
    dh_acc[...] = jnp.zeros_like(dh_acc)
    for j in range(chunks):
        at_first(j)
        pre = dot(h_two, w_fc1[:, cols(j)]) + b_fc1[:, cols(j)]
        cdf = 0.5 + 0.5 * lax.erf(pre * (0.5 ** 0.5))
        pdf = jnp.exp(pre * pre * -0.5) * 0.3989422804014327
        act = (pre * cdf).astype(BF16)
        d_act = dot(dy, w_fc2[cols(j), :], NT)
        d_pre = d_act * (cdf + pre * pdf)
        y_acc[...] += dot(act, w_fc2[cols(j), :])
        gw_fc2[cols(j), :] += dot(act, dy, TN)
        g_b1[:, cols(j)] += col_sum(d_pre)
        d_pre = d_pre.astype(BF16)
        gw_fc1[j] += dot(h_two, d_pre, TN)
        dh_acc[...] += dot(d_pre, w_fc1[:, cols(j)], NT)
        if j > 0:
            at_last(j - 1)
    at_last(chunks - 1)
    y_out[...] = y_acc[...].astype(BF16)
    d_two = dh_acc[...]
    dy_f = dy.astype(F32)
    d_mid = dy_f + hat_bwd(d_two, x_hat, inv_std, gain)
    dmid_out[...] = d_mid
    for row, grad in enumerate((d_mid, d_two * x_hat, d_two, dy_f)):
        g_small[row:row + 1, :] += col_sum(grad)
    d_mid = d_mid.astype(BF16)
    gw_out[...] += dot(ctx_val, d_mid, TN)
    dctx_out[...] = dot(d_mid, w_out[...], NT).astype(BF16)
    at_last(chunks)

    @pl.when(step == pl.num_programs(0) - 1)
    def _():
        for j in range(chunks + 1):
            for copy in stores(j):
                copy.wait()


def whole(shape):
    return pl.BlockSpec(shape, lambda *_: (0,) * len(shape), pipeline_mode=pl.Buffered(1))


def shape_of(dims, dtype):
    return jax.ShapeDtypeStruct(dims, dtype)


def call(kernel, grid, in_specs, out_specs, out_shape, args, flops, scratch=(), name=None, collective_id=None):
    moved = sum(a.size * a.dtype.itemsize for a in args) + sum(o.size * o.dtype.itemsize for o in out_shape)
    return pl.pallas_call(
        kernel, grid=grid, in_specs=in_specs, out_specs=out_specs, out_shape=out_shape,
        scratch_shapes=list(scratch), name=name,
        compiler_params=pltpu.CompilerParams(vmem_limit_bytes=VMEM_LIMIT,
                                             dimension_semantics=('arbitrary',) * len(grid),
                                             collective_id=collective_id,
                                             has_side_effects=collective_id is not None),
        cost_estimate=pl.CostEstimate(flops=flops, bytes_accessed=moved, transcendentals=0))(*args)


def layer_compute(tokens, grad_y, vec_part, weights):
    seqs, seq_len = tokens.shape
    dim, ff = grad_y.shape[2], weights[2].shape[1]
    n_tok, pairs, half = seqs * seq_len, dim // PAIR, dim // 2
    cos, sin = rope_tables(seq_len)
    tok_seq = tokens.reshape(seqs, 1, seq_len)
    any_spec = pl.BlockSpec(memory_space=pl.ANY)
    wide = shape_of((n_tok, dim), BF16)
    wide_f32 = shape_of((n_tok, dim), F32)

    def rows_spec(rows, width=dim):
        return pl.BlockSpec((rows, width), lambda i: (i, 0))

    def wholes(*arrays):
        return [whole(a.shape) for a in arrays]

    def sems(*counts):
        return [pltpu.SemaphoreType.DMA((n,)) for n in counts]

    tile = 256
    per_seq = seq_len // tile
    table_spec = pl.BlockSpec((tile, PAIR), lambda i: (i % per_seq, 0))
    full = [shape_of((2 * w.shape[0],) + w.shape[1:], BF16) for w in weights]
    vec_shape = shape_of((2,) + vec_part.shape, BF16)
    x_in, q, k, v, vec, w_qkv, w_out, w_fc1, w_fc2 = call(
        qkv_kernel, (n_tok // tile,),
        [pl.BlockSpec((1, 1, seq_len), lambda i: (i // per_seq, 0, 0)),
         any_spec, table_spec, table_spec] + [any_spec] * 4,
        [rows_spec(tile)] * 4 + wholes(vec_shape) + [any_spec] * 4, [wide] * 4 + [vec_shape] + full,
        (tok_seq, vec_part, cos, sin) + tuple(weights),
        6 * n_tok * dim * dim,
        scratch=[pltpu.VMEM(full[0].shape, BF16), pltpu.VMEM(vec_shape.shape, BF16)]
        + [pltpu.VMEM(w.shape, BF16) for w in weights[1:]] + sems(5, 5, 9), name='qkv', collective_id=2)

    head_spec = pl.BlockSpec((seq_len, PAIR), lambda b, p: (b, p))
    tok_spec = pl.BlockSpec((1, 1, seq_len), lambda b, p: (b, 0, 0))
    lse_spec = pl.BlockSpec((1, 2, seq_len), lambda b, p: (b * pairs + p, 0, 0))
    ctx, lse = call(
        attn_fwd_kernel, (seqs, pairs), [head_spec] * 3 + [tok_spec], [head_spec, lse_spec],
        [wide, shape_of((seqs * pairs, 2, seq_len), F32)],
        (q, k, v, tok_seq), 16 * n_tok * seq_len * dim, name='attn_fwd')

    tile = 512
    pages = shape_of((ff // dim, dim, dim), F32)
    grads = [shape_of(w_out.shape, F32), pages, shape_of(w_fc2.shape, F32), shape_of((8, dim), F32),
             shape_of((1, ff), F32)]
    hidden, d_mid, d_ctx, gw_out, gw_fc1, gw_fc2, small_two, g_b1 = call(
        ffn_kernel, (n_tok // tile,), [rows_spec(tile)] * 3 + [any_spec] * 3 + wholes(vec),
        [rows_spec(tile)] * 3 + [any_spec] * 3 + wholes(*grads[3:]), [wide, wide_f32, wide] + grads,
        (ctx, x_in, grad_y.reshape(n_tok, dim), w_out, w_fc1, w_fc2, vec),
        6 * n_tok * dim * (dim + 2 * ff), scratch=[pltpu.VMEM((tile, dim), F32)] * 2 + [pltpu.VMEM(w.shape, BF16) for w in (w_out, w_fc1, w_fc2)]
        + [pltpu.VMEM(g.shape, F32) for g in grads[:3]] + [pltpu.VMEM((1, ff), F32)] + sems(2 * ff // dim + 1), name='ffn')

    blocks = (3, RING, RING, half // (3 * RING * RING), dim)
    whole_table = pl.BlockSpec((seq_len, PAIR), lambda b, p: (0, 0))
    red_shape = shape_of((3, 2) + blocks[3:], F32)
    sum_shape = shape_of((seqs * pairs, 3, PAIR), F32)
    n_sems = 2 + 12 * SCATTER_SEMS
    dq, dk, dv, b_sums, red = call(
        attn_bwd_reduce_kernel, (seqs, pairs),
        [head_spec] * 4 + [lse_spec, tok_spec, whole_table, whole_table, any_spec, any_spec],
        [head_spec] * 3 + [pl.BlockSpec((1, 3, PAIR), lambda b, p: (b * pairs + p, 0, 0))] + wholes(red_shape),
        [wide] * 3 + [sum_shape, red_shape],
        (q, k, v, d_ctx, lse, tok_seq, cos, sin, gw_fc2.reshape((2, RING) + blocks), gw_fc1.reshape((RING, 2) + blocks)),
        40 * n_tok * seq_len * dim,
        scratch=[pltpu.VMEM((RING, 2) + blocks, F32)] * 2
        + comm_temps(2, blocks[3], dim) + sems(n_sems, n_sems, 2), name='attn_bwd', collective_id=0)

    n_sems = 16 + 18 * FLOW_SEMS
    fc2, fc1, out, qkv, small_sum = call(
        qkv_bwd_reduce_kernel, (seqs,),
        [pl.BlockSpec((1, 1, seq_len), lambda i: (i, 0, 0))] + [rows_spec(seq_len)] * 5
        + wholes(w_qkv, vec, red, small_two, g_b1, b_sums) + [any_spec],
        [any_spec] * 4 + [whole((SMALL_ROWS, half))],
        [shape_of((RING,) + blocks, F32), shape_of(blocks[:-1] + (ff,), F32), shape_of(blocks, F32),
         shape_of(blocks[:-1] + (3 * dim,), F32), shape_of((SMALL_ROWS, half), F32)],
        (tok_seq, x_in, dq, dk, dv, d_mid, w_qkv, vec, red, small_two, g_b1, b_sums, gw_out.reshape((2,) + blocks)),
        12 * n_tok * dim * dim,
        scratch=[pltpu.VMEM((RING, 2) + blocks, F32), pltpu.VMEM((RING, 1) + blocks, F32)]
        + comm_temps(1, blocks[3], dim)
        + [pltpu.VMEM((RING, 2) + blocks, F32), pltpu.VMEM((2, SMALL_ROWS, half), F32),
           pltpu.VMEM((SMALL_ROWS, half), F32), pltpu.VMEM((3, RING, SMALL_ROWS, half), F32)]
        + sems(n_sems, n_sems, 10), name='qkv_bwd', collective_id=1)
    big = (qkv.reshape(half, 3 * dim), out.reshape(half, dim), fc1.reshape(half, ff), fc2.reshape(ff // 2, dim))
    return hidden.reshape(grad_y.shape), big, small_sum


RING = 4
ALL = slice(None)
DIRECT = 2
ORDERS = ('xyz', 'yzx', 'zxy')
STRIDE = {'x': 1, 'y': RING, 'z': RING * RING}
MESH_ID = pl.DeviceIdType.MESH


class Torus:
    def __init__(self):
        self.me = lax.axis_index('dp')
        self.part = lax.axis_index('fsdp')
        self.coord = {axis: self.me // stride % RING for axis, stride in STRIDE.items()}

    def at(self, axis, delta):
        return (self.coord[axis] + delta + RING) % RING

    def chip(self, axis, delta):
        return {'dp': self.me + (self.at(axis, delta) - self.coord[axis]) * STRIDE[axis]}

    def partner(self):
        return {'fsdp': 1 - self.part}

    def greet(self):
        barrier = pltpu.get_barrier_semaphore()
        peers = [self.partner()] + [self.chip(axis, delta) for axis in 'xyz' for delta in (1, -1, 2)]
        for peer in peers:
            pl.semaphore_signal(barrier, inc=1, device_id=peer, device_id_type=MESH_ID)
        pl.semaphore_wait(barrier, len(peers))


class Flow:
    def __init__(self, torus, order, sign, view, temp_view, grads, sums, temps, sends, recvs, base):
        self.torus, self.order, self.sign = torus, order, sign
        self.view, self.temp_view = view, temp_view
        self.grads, self.sums, self.temps = grads, sums, temps
        self.sends, self.recvs, self.base = sends, recvs, base
        self.used = []

    def route(self, slot):
        level, kind = slot % 9 // 3, slot % 3
        sign = self.sign
        if slot < 9:
            target = self.temp_view(self.temps, level, kind)
            if kind == 2 and level != DIRECT:
                return self.temp_view(self.temps, level, 0), target, level, sign
            delta = (2, -sign, sign)[kind]
            return self.view(self.grads, self.place(level, delta)), target, level, delta if level == DIRECT or kind else sign
        if kind == 2 and level != DIRECT:
            block = self.view(self.sums, self.place(level, -sign))
            return block, block, level, sign
        target = self.view(self.sums, self.place(level + 1))
        source = self.final(self) if level == DIRECT else target
        return source, target, level, (sign, -sign, 2)[kind]

    def copy(self, slot):
        src, dst, level, delta = self.route(slot)
        return pltpu.make_async_remote_copy(
            src_ref=src, dst_ref=dst, send_sem=self.sends.at[self.base + slot],
            recv_sem=self.recvs.at[self.base + slot],
            device_id=self.torus.chip(self.order[level], delta), device_id_type=MESH_ID)

    def start(self, slot):
        self.used.append(slot)
        self.copy(slot).start()

    def wait(self, slot):
        self.copy(slot).wait_recv()

    def place(self, level, delta=None):
        own = [self.torus.coord[axis] for axis in self.order[:level]]
        return tuple(own) + (() if delta is None else (self.torus.at(self.order[level], delta),))

    def start_level(self, first, level):
        for kind in range(3 if level == DIRECT else 2):
            self.start(first + kind)

    def wait_level(self, first, level):
        for kind in range(0 if level == DIRECT else 1, 3):
            self.wait(first + kind)

    def scatter_start(self, level):
        self.start_level(level * 3, level)

    def scatter_mid(self, level):
        if level == DIRECT:
            return
        self.wait(level * 3)
        relay = self.temp_view(self.temps, level, 0)
        relay[...] = relay[...] + self.view(self.grads, self.place(level, self.sign))[...]
        self.start(level * 3 + 2)

    def scatter_end(self, level):
        self.wait_level(level * 3, level)
        mine = self.view(self.grads, self.place(level, 0))
        total = mine[...]
        for kind in range(0 if level == DIRECT else 1, 3):
            total = total + self.temp_view(self.temps, level, kind)[...]
        mine[...] = total

    def gather_start(self, level):
        if level == DIRECT:
            self.view(self.sums, self.place(3))[...] = self.final(self)[...]
        self.start_level(9 + level * 3, level)

    def gather_mid(self, level):
        if level == DIRECT:
            return
        self.wait(9 + level * 3)
        self.start(11 + level * 3)

    def gather_end(self, level):
        self.wait_level(9 + level * 3, level)

    def scatter_next(self, level):
        self.scatter_end(level)
        if level == DIRECT:
            self.gather_start(level)
        else:
            self.scatter_start(level + 1)

    def gather_next(self, level):
        self.gather_end(level)
        self.gather_start(level - 1)

    def finish(self):
        for slot in self.used:
            self.copy(slot).wait_send()


FLOW_SEMS = 18
SCATTER_SEMS = 9


def own_block(flow):
    return flow.view(flow.grads, flow.place(3))


def make_flows(torus, width, grads, sums, temps, sends, recvs, base, group=ALL, temp_group=ALL, final=own_block,
               spacing=FLOW_SEMS, pieces=None):
    half = width // 2
    flows = []
    for first, size in pieces or ((0, half),):
        for color, order, side in [(color, order, side) for color, order in enumerate(ORDERS) for side in range(2)]:
            sign = 1 - 2 * side
            lanes = pl.ds(side * half + first, size)

            def view(ref, place, color=color, lanes=lanes):
                rest = place[1:] + (ALL,) * (4 - len(place))
                return ref.at[(place[0], group if ref is grads else ALL, color) + rest + (lanes,)]

            def temp_view(refs, level, kind, color=color, lanes=lanes):
                return refs[level].at[(kind, temp_group, color) + (ALL,) * (3 - level) + (lanes,)]

            flow = Flow(torus, order, sign, view, temp_view, grads, sums, temps, sends, recvs,
                        base + len(flows) * spacing)
            flow.final, flow.color, flow.lanes = final, color, lanes
            flows.append(flow)
    return flows


def each(flows, name, level):
    for flow in flows:
        getattr(flow, name)(level)


def comm_temps(groups, rows, dim):
    return [pltpu.VMEM((3, groups, 3) + (RING,) * (2 - level) + (rows, dim), F32) for level in range(3)]


PLAN = ('b', '', 'e0', '', 'e1', 'm00', '', 'm10', 'a00', 'm01 a10', 'a01 m11', 'a11', 'a02 a12')


def attn_bwd_reduce_kernel(q, k, v, d_ctx, lse, tok_seq, cos, sin, fc2, fc1, dq_out, dk_out, dv_out, sums_out, red,
                           grads, other_sum, temp0, temp1, temp2, sends, recvs, local):
    torus = Torus()
    step = pl.program_id(0) * pl.num_programs(1) + pl.program_id(1)
    sets = [make_flows(torus, grads.shape[-1], grads, None, (temp0, temp1, temp2), sends, recvs,
                       2 + n * 6 * SCATTER_SEMS, group=pl.ds(n, 1), temp_group=pl.ds(n, 1), spacing=SCATTER_SEMS)
            for n in range(2)]
    sources = (lambda i: fc2.at[i], lambda i: fc1.at[:, i])

    def remote(n):
        return pltpu.make_async_remote_copy(
            src_ref=sources[n](1 - torus.part), dst_ref=other_sum.at[:, n], send_sem=sends.at[n], recv_sem=recvs.at[n],
            device_id=torus.partner(), device_id_type=MESH_ID)

    def mine(n):
        return pltpu.make_async_copy(sources[n](torus.part), grads.at[:, n], local.at[n])

    def begin():
        torus.greet()
        for n in range(2):
            remote(n).start()
            mine(n).start()

    def enter(n):
        remote(n).wait_recv()
        mine(n).wait()

        @pl.loop(0, RING)
        def _(page):
            grads[page, n] = grads[page, n] + other_sum[page, n]
        each(sets[n], 'scatter_start', 0)

    def mid(n, level):
        each(sets[n], 'scatter_mid', level)

    def after(n, level):
        each(sets[n], 'scatter_next' if level < 2 else 'scatter_end', level)

    actions = {'b': begin, 'e': enter, 'm': mid, 'a': after}

    def perform(words):
        for word in words.split():
            actions[word[0]](*(int(number) for number in word[1:]))

    for at_step, words in enumerate(PLAN[:-1]):
        pl.when(step == at_step)(functools.partial(perform, words))

    attn_bwd_kernel(q, k, v, d_ctx, lse, tok_seq, cos, sin, dq_out, dk_out, dv_out, sums_out)

    @pl.when(step == len(PLAN) - 2)
    def _():
        perform(PLAN[-1])
        for n, flows in enumerate(sets):
            for flow in flows:
                red[flow.color, n:n + 1, :, flow.lanes] = own_block(flow)[...]
                flow.finish()
            remote(n).wait_send()


def qkv_bwd_reduce_kernel(tok_seq, x_in, dq, dk, dv, d_mid, w_qkv, vec, red, small_two, g_b1, b_sums,
                          gw_out, fc2_sum, fc1_sum, out_sum, qkv_sum, small_sum,
                          grads, sums, temp0, temp1, temp2, sums_ab, small, small_other, small_slots,
                          sends, recvs, local):
    torus = Torus()
    step = pl.program_id(0)
    last = pl.num_programs(0) - 1
    dim = x_in.shape[1]
    half = dim // 2
    part = torus.part

    def final(flow):
        return red.at[flow.color, :, :, flow.lanes]

    gathers = make_flows(torus, dim, None, sums_ab, None, sends, recvs, 16, final=final)
    flows = make_flows(torus, dim, grads, sums, (temp0, temp1, temp2), sends, recvs, 16 + 6 * FLOW_SEMS,
                       group=pl.ds(part, 1), pieces=((0, 2 * PAIR), (2 * PAIR, PAIR)))

    def load_out():
        return pltpu.make_async_copy(gw_out, grads.at[0], local.at[0])

    def later_hook():
        each(gathers, 'gather_next', 2)
        each(gathers, 'gather_mid', 1)

    def last_hook():
        each(gathers, 'gather_next', 1)
        load_out().wait()

    hooks = ((0, 1, lambda: each(gathers, 'gather_mid', 2)), (0, 2, later_hook), (1, 0, last_hook))

    def pair_copy(page):
        return pltpu.make_async_remote_copy(
            src_ref=grads.at[page, 1 - part], dst_ref=sums.at[page, 0], send_sem=sends.at[1 + page],
            recv_sem=recvs.at[1 + page], device_id=torus.partner(), device_id_type=MESH_ID)

    @pl.when(step == 0)
    def _():
        torus.greet()
        load_out().start()
        each(gathers, 'gather_start', 2)
        small[...] = jnp.zeros_like(small)
        for page in range(1, RING):
            grads[page] = jnp.zeros(grads.shape[1:], F32)

    x_hat, inv_std = hat_of(x_in[...].astype(F32))
    gain = vec_row(vec, 'ln1_gain')
    h_one = (x_hat * gain + vec_row(vec, 'ln1_bias')).astype(BF16)
    d_one = None
    for index, ref in enumerate((dq, dk, dv)):
        for at_step, at_index, hook in hooks:
            if at_index == index:
                pl.when(step == at_step)(hook)
        cols = slice(index * dim, (index + 1) * dim)
        d_part = ref[...]
        grads[index + 1] += dot(h_one, d_part, TN).reshape(grads.shape[1:])
        new = dot(d_part, w_qkv[:, cols], NT)
        pl.when(step == last)(pair_copy(index).start)
        d_one = new if index == 0 else d_one + new
    g_rows = jnp.concatenate([col_sum(d_one * x_hat), col_sum(d_one)], axis=0)
    d_in = d_mid[...] + hat_bwd(d_one, x_hat, inv_std, gain)
    scale, _ = seq_counts(tok_seq[0])
    one_hot = live_one_hot(tok_seq[0], EMB_ROWS)
    high = d_in.astype(BF16)
    low = (d_in - high.astype(F32)).astype(BF16)
    g_emb = (dot(one_hot, high) + dot(one_hot, low)) * scale
    for side in range(2):
        lanes = slice(side * half, (side + 1) * half)
        small[side, :EMB_ROWS, :] += g_emb[:, lanes]
        small[side, EMB_ROWS:EMB_ROWS + 2, :] += g_rows[:, lanes]

    @pl.when(step == last)
    def _():
        pair_copy(RING - 1).start()
        pairs = dim // PAIR
        per_pair = [b_sums[p] for p in range(pairs)]
        for b in range(1, b_sums.shape[0] // pairs):
            per_pair = [per_pair[p] + b_sums[b * pairs + p] for p in range(pairs)]
        b_qkv = jnp.concatenate([per_pair[p][i:i + 1] for i in range(3) for p in range(pairs)], axis=1)
        for side in range(2):
            row = EMB_ROWS + 2
            small[side, row:row + 4, :] = small_two[:4, side * half:(side + 1) * half]
            row += 4
            for grad in (b_qkv, g_b1[...]):
                base = side * (grad.shape[1] // 2)
                for i in range(grad.shape[1] // dim):
                    small[side, row:row + 1, :] = grad[:, base + i * half:base + (i + 1) * half]
                    row += 1
        small_copy = pltpu.make_async_remote_copy(
            src_ref=small.at[1 - part], dst_ref=small_other, send_sem=sends.at[0], recv_sem=recvs.at[0],
            device_id=torus.partner(), device_id_type=MESH_ID)
        small_copy.start()
        started = [small_copy] + [pair_copy(page) for page in range(RING)]

        def small_start(level, value):
            axis = ORDERS[0][level]
            here = torus.coord[axis]
            small_slots[level, here] = value
            slot = small_slots.at[level, here]
            copies = [pltpu.make_async_remote_copy(
                src_ref=slot, dst_ref=slot, send_sem=sends.at[5 + level * 3 + n], recv_sem=recvs.at[5 + level * 3 + n],
                device_id=torus.chip(axis, delta), device_id_type=MESH_ID) for n, delta in enumerate((1, -1, 2))]
            for copy in copies:
                copy.start()
            started.extend(copies)
            return copies

        def small_end(level, copies):
            for copy in copies:
                copy.wait_recv()
            return ((small_slots[level, 0] + small_slots[level, 1]) + small_slots[level, 2]) + small_slots[level, 3]

        small_copy.wait_recv()
        small_copies = small_start(0, small[part] + small_other[...])
        for page in range(RING):
            started[1 + page].wait_recv()

            @pl.loop(0, 3)
            def _(i):
                grads[page, part, i] = grads[page, part, i] + sums[page, 0, i]
        each(flows, 'scatter_start', 0)
        each(gathers, 'gather_mid', 0)
        for level in range(3):
            each(flows, 'scatter_mid', level)
            total = small_end(level, small_copies)
            if level < 2:
                small_copies = small_start(level + 1, total)
            each(flows, 'scatter_next', level)
        small_sum[...] = total
        each(gathers, 'gather_end', 0)
        stores = [pltpu.make_async_copy(sums_ab.at[:, 0], fc2_sum, local.at[1])]
        for page in range(RING):
            lanes = pl.ds(page * dim, dim)
            stores.append(pltpu.make_async_copy(sums_ab.at[page, 1], fc1_sum.at[:, :, :, :, lanes], local.at[2 + page]))
        for store in stores:
            store.start()
        each(flows, 'gather_mid', 2)
        for level in (1, 0):
            each(flows, 'gather_next', level + 1)
            each(flows, 'gather_mid', level)
        each(flows, 'gather_end', 0)
        tail = [pltpu.make_async_copy(sums.at[0, 0], out_sum, local.at[6])]
        for page in range(3):
            tail.append(pltpu.make_async_copy(
                sums.at[page + 1, 0], qkv_sum.at[:, :, :, :, pl.ds(page * dim, dim)], local.at[7 + page]))
        for store in tail:
            store.start()
        for copy in started:
            copy.wait_send()
        for flow in gathers + flows:
            flow.finish()
        for store in stores + tail:
            store.wait()


def solution(mesh):
    row_spec = P(('dp', 'fsdp'), None)
    act_spec = P(('dp', 'fsdp'), None, None)
    param_specs = (P(None, 'fsdp'),) + (P('fsdp'),) * 12

    def local_step(tokens, grad_y, *shards):
        (embedding, ln1_gain, ln1_bias, w_qkv, b_qkv, w_out, b_out,
         ln2_gain, ln2_bias, w_fc1, b_fc1, w_fc2, b_fc2) = shards
        vectors = (ln1_gain, ln1_bias, b_out, ln2_gain, ln2_bias, b_fc2, b_qkv, b_fc1)
        vocab, width = embedding.shape
        rows = [vec[first:first + width] for vec in vectors for first in range(0, vec.size, width)]
        at_row = jnp.asarray(np.indices((SMALL_ROWS, width))[0], jnp.int32)
        vec_part = jnp.pad(embedding, ((0, SMALL_ROWS - vocab), (0, 0)))
        for index, row in enumerate(rows):
            vec_part = jnp.where(at_row == VEC_ROW + index, row[None, :], vec_part)
        hidden, big, small_sum = layer_compute(tokens, grad_y, vec_part, (w_qkv, w_out, w_fc1, w_fc2))
        g_w_qkv, g_w_out, g_w_fc1, g_w_fc2 = big
        g_embedding = small_sum[:vocab]
        start = EMB_ROWS
        vec_grads = []
        for vec in vectors:
            stop = start + vec.size // width
            vec_grads.append(small_sum[start:stop].reshape(-1))
            start = stop
        (g_ln1_gain, g_ln1_bias, g_b_out, g_ln2_gain, g_ln2_bias, g_b_fc2, g_b_qkv, g_b_fc1) = vec_grads
        return (hidden, g_embedding, g_ln1_gain, g_ln1_bias, g_w_qkv, g_b_qkv, g_w_out, g_b_out,
                g_ln2_gain, g_ln2_bias, g_w_fc1, g_b_fc1, g_w_fc2, g_b_fc2)

    return jax.shard_map(local_step, mesh=mesh, in_specs=(row_spec, act_spec) + param_specs,
                         out_specs=(act_spec,) + param_specs, check_vma=False)
```

```python
import functools
import jax
import jax.numpy as jnp
import numpy as np
from jax import lax
from jax.experimental import pallas as pl
from jax.experimental.pallas import tpu as pltpu
from jax.sharding import PartitionSpec as P

HEAD_DIM = 64
MASK_ID = 32
PAD_ID = 1
MASK_RATIO = 0.15 * 0.8
LN_EPS = 1e-5
ROPE_BASE = 10000.0
F32 = jnp.float32
BF16 = jnp.bfloat16
EMB_ROWS = 40
SMALL_ROWS = 64
VEC_ROW = 48
VECTORS = ('ln1_gain', 'ln1_bias', 'b_out', 'ln2_gain', 'ln2_bias', 'b_fc2', 'b_qkv', 'b_fc1')
SCALE = HEAD_DIM ** -0.5
VMEM_LIMIT = 60 << 20

NN = (((1,), (0,)), ((), ()))
NT = (((1,), (1,)), ((), ()))
TN = (((0,), (0,)), ((), ()))


def dot(lhs, rhs, dims=NN):
    return lax.dot_general(lhs, rhs, dims, preferred_element_type=F32)


def row_mean(x_val):
    return jnp.mean(x_val, axis=-1, keepdims=True)


def hat_of(x_val):
    centered = x_val - row_mean(x_val)
    inv_std = lax.rsqrt(row_mean(centered * centered) + LN_EPS)
    return centered * inv_std, inv_std


def hat_bwd(d_out, x_hat, inv_std, gain):
    d_hat = d_out * gain
    return inv_std * (d_hat - row_mean(d_hat)
                      - x_hat * row_mean(d_hat * x_hat))


def rope_tables(seq_len):
    power = np.arange(0, HEAD_DIM, 2, dtype=np.float32) / np.float32(HEAD_DIM)
    inv_freq = np.float32(1) / np.power(np.float32(ROPE_BASE), power)
    angles = np.outer(np.arange(seq_len, dtype=np.float32), inv_freq).astype(np.float64)
    cos, sin = np.cos(angles), np.sin(angles)
    return (jnp.asarray(np.concatenate([cos] * 4, axis=1), F32),
            jnp.asarray(np.concatenate([-sin, sin] * 2, axis=1), F32))


def col_sum(x_val):
    return jnp.sum(x_val, axis=0, keepdims=True)


def iota(shape, dim):
    return lax.broadcasted_iota(jnp.int32, shape, dim)


def vec_row(vec, name):
    at = VECTORS.index(name)
    count = {'b_qkv': 3, 'b_fc1': 4}.get(name, 1)
    row = VEC_ROW + at + (2 if name == 'b_fc1' else 0)
    return jnp.concatenate([vec[side, i:i + 1, :] for side in range(2) for i in range(row, row + count)],
                           axis=1).astype(F32)


def seq_counts(tok_row):
    masks = jnp.sum((tok_row == MASK_ID).astype(F32), axis=1, keepdims=True)
    real = jnp.sum((tok_row != PAD_ID).astype(F32), axis=1, keepdims=True)
    return (1.0 - MASK_RATIO) / (1.0 - masks / real), real


def live_one_hot(tok_row, rows):
    live = (tok_row == iota((rows, tok_row.shape[1]), 0)) & (tok_row != MASK_ID) & (tok_row != PAD_ID)
    return live.astype(F32).astype(BF16)


def swap_halves(x_val):
    low = (iota(x_val.shape, 1) & 32) == 0
    return jnp.where(low, pltpu.roll(x_val, 96, 1), pltpu.roll(x_val, 32, 1))


def rows_of_head(x_val, head):
    return jnp.where((iota(x_val.shape, 0) >= HEAD_DIM) == (head == 1), x_val, jnp.zeros_like(x_val))


def lanes_of_head(x_val, head):
    return jnp.where((iota(x_val.shape, 1) >= HEAD_DIM) == (head == 1), x_val, jnp.zeros_like(x_val))


def qkv_kernel(tok_seq, vec_part, cos, sin, wq_part, wo_part, w1_part, w2_part,
               x_out, q_out, k_out, v_out, vec_out, wq_out, wo_out, w1_out, w2_out,
               w_qkv, vec, wo_own, w1_own, w2_own, sends, recvs, local):
    step = pl.program_id(0)
    part = lax.axis_index('fsdp')
    partner = {'fsdp': 1 - part}
    dim = x_out.shape[1]

    def own_rows(ref):
        size = ref.shape[0] // 2
        return ref.at[pl.ds(part * size, size)]

    moves = [(wq_part, w_qkv), (vec_part, vec.at[part]), (wo_own, wo_out), (w1_own, w1_out), (w2_own, w2_out)]

    def target(n):
        return moves[n][1] if n == 1 else own_rows(moves[n][1])

    def remote(n):
        return pltpu.make_async_remote_copy(
            src_ref=moves[n][0], dst_ref=target(n), send_sem=sends.at[n], recv_sem=recvs.at[n],
            device_id=partner, device_id_type=MESH_ID)

    def keep_own(n):
        return pltpu.make_async_copy(moves[n][0], target(n), local.at[n])

    stage = ((wo_part, wo_own), (w1_part, w1_own), (w2_part, w2_own))

    def store_qkv():
        return pltpu.make_async_copy(w_qkv, wq_out, local.at[len(moves) + len(stage)])

    @pl.when(step == 0)
    def _():
        barrier = pltpu.get_barrier_semaphore()
        pl.semaphore_signal(barrier, inc=1, device_id=partner, device_id_type=MESH_ID)
        pl.semaphore_wait(barrier, 1)
        for n in range(2):
            remote(n).start()
            keep_own(n).start()
        loads = [pltpu.make_async_copy(src, dst, local.at[len(moves) + n]) for n, (src, dst) in enumerate(stage)]
        for copy in loads:
            copy.start()
        for n, copy in enumerate(loads):
            copy.wait()
            remote(n + 2).start()
            keep_own(n + 2).start()
        for n in range(2):
            remote(n).wait_recv()
            keep_own(n).wait()
        store_qkv().start()
        vec_out[...] = vec[...]

    per_seq = tok_seq.shape[2] // x_out.shape[0]
    first = lax.rem(step, per_seq) * x_out.shape[0]
    tok_tile = tok_seq[0, :, pl.ds(pl.multiple_of(first, x_out.shape[0]), x_out.shape[0])]
    scale, _ = seq_counts(tok_seq[0])
    emb = jnp.concatenate([vec[side, :VEC_ROW, :] for side in range(2)], axis=1)
    x_b16 = (dot(live_one_hot(tok_tile, VEC_ROW), emb, TN) * scale).astype(BF16)
    x_out[...] = x_b16
    x_hat, _ = hat_of(x_b16.astype(F32))
    h_one = (x_hat * vec_row(vec, 'ln1_gain') + vec_row(vec, 'ln1_bias')).astype(BF16)
    cos_tab, sin_tab = cos[...], sin[...]
    b_qkv = vec_row(vec, 'b_qkv')
    for index, out in enumerate((q_out, k_out, v_out)):
        cols = slice(index * dim, (index + 1) * dim)
        proj = dot(h_one, w_qkv[:, cols]) + b_qkv[:, cols]
        if out is v_out:
            out[...] = proj.astype(BF16)
            continue
        if out is q_out:
            proj = proj * SCALE
        for first in range(0, dim, PAIR):
            pair = slice(first, first + PAIR)
            z = proj[:, pair]
            out[:, pair] = (z * cos_tab + swap_halves(z) * sin_tab).astype(BF16)

    @pl.when(step == pl.num_programs(0) - 1)
    def _():
        store_qkv().wait()
        for n in range(len(moves)):
            remote(n).wait_send()
            if n >= 2:
                remote(n).wait_recv()
                keep_own(n).wait()


PAIR = 2 * HEAD_DIM
def pad_bias(tok_row):
    _, real = seq_counts(tok_row)
    size = tok_row.shape[1]
    return jnp.where(iota((size, size), 0).astype(F32) < real, 0.0, -1e30)


def head_rows(head):
    return slice(head * HEAD_DIM, (head + 1) * HEAD_DIM)


def attn_fwd_kernel(q, k, v, tok_seq, ctx, lse):
    q_t, v_t, k_val = q[...].T, v[...].T, k[...]
    bias = pad_bias(tok_seq[0])
    parts = []
    for head in range(2):
        s_t = dot(k_val, rows_of_head(q_t, head)) + bias
        top = jnp.max(s_t, axis=0, keepdims=True)
        e_t = jnp.exp(s_t - top)
        total = col_sum(e_t)
        lse[0, head:head + 1, :] = top + jnp.log(total)
        p_t = (e_t * (1.0 / total)).astype(BF16)
        parts.append(dot(v_t[head_rows(head), :], p_t))
    ctx[...] = jnp.concatenate(parts, axis=0).T.astype(BF16)


def attn_bwd_kernel(q, k, v, d_ctx, lse, tok_seq, cos, sin, dq_out, dk_out, dv_out, sums):
    q_val, k_val, v_val, d_val = q[...], k[...], v[...], d_ctx[...]
    q_t, k_t, d_t = q_val.T, k_val.T, d_val.T
    bias = pad_bias(tok_seq[0])
    parts, d_key, d_value = [], 0.0, 0.0
    for head in range(2):
        s_t = dot(k_val, rows_of_head(q_t, head)) + bias
        p_t = jnp.exp(s_t - lse[0, head:head + 1, :])
        dp_t = dot(v_val, rows_of_head(d_t, head))
        delta = col_sum(p_t * dp_t)
        ds_t = (p_t * (dp_t - delta)).astype(BF16)
        d_value += dot(p_t.astype(BF16), lanes_of_head(d_val, head))
        d_key += dot(ds_t, lanes_of_head(q_val, head))
        parts.append(dot(k_t[head_rows(head), :], ds_t))

    def unrotate(z):
        return z * cos[...] - swap_halves(z) * sin[...]

    grads = (unrotate(jnp.concatenate(parts, axis=0).T) * SCALE, unrotate(d_key), d_value)
    for grad, out in zip(grads, (dq_out, dk_out, dv_out)):
        out[...] = grad.astype(BF16)
    sums[0] = jnp.concatenate([col_sum(grad) for grad in grads], axis=0)


FF_CHUNK = 768


def ffn_kernel(ctx, x_in, grad_y, wo_hbm, w1_hbm, w2_hbm, vec,
               y_out, dmid_out, dctx_out, gwo_hbm, gw1_hbm, gw2_hbm, g_small, g_b1,
               y_acc, dh_acc, w_out, w_fc1, w_fc2, gw_out, gw_fc1, gw_fc2, b_fc1, local):
    step = pl.program_id(0)
    chunks = w_fc1.shape[1] // FF_CHUNK

    def cols(j):
        return pl.ds(j * FF_CHUNK, FF_CHUNK)

    def loads(j):
        if j == chunks:
            return [pltpu.make_async_copy(wo_hbm, w_out, local.at[2 * j])]
        return [pltpu.make_async_copy(w1_hbm.at[:, cols(j)], w_fc1.at[:, cols(j)], local.at[2 * j]),
                pltpu.make_async_copy(w2_hbm.at[cols(j)], w_fc2.at[cols(j)], local.at[2 * j + 1])]

    def stores(j):
        if j == chunks:
            return [pltpu.make_async_copy(gw_out, gwo_hbm, local.at[2 * j])]
        return [pltpu.make_async_copy(gw_fc1.at[j], gw1_hbm.at[j], local.at[2 * j]),
                pltpu.make_async_copy(gw_fc2.at[cols(j)], gw2_hbm.at[cols(j)], local.at[2 * j + 1])]

    def at_first(j):
        @pl.when(step == 0)
        def _():
            for copy in loads(j):
                copy.wait()

    def at_last(j):
        @pl.when(step == pl.num_programs(0) - 1)
        def _():
            for copy in stores(j):
                copy.start()

    @pl.when(step == 0)
    def _():
        for j in [chunks] + list(range(chunks)):
            for copy in loads(j):
                copy.start()
        for ref in (gw_out, gw_fc1, gw_fc2, g_small, g_b1):
            ref[...] = jnp.zeros_like(ref)
        b_fc1[...] = vec_row(vec, 'b_fc1')

    gain = vec_row(vec, 'ln2_gain')
    ctx_val = ctx[...]
    at_first(chunks)
    x_mid = x_in[...].astype(F32) + dot(ctx_val, w_out[...]) + vec_row(vec, 'b_out')
    x_hat, inv_std = hat_of(x_mid)
    h_two = (x_hat * gain + vec_row(vec, 'ln2_bias')).astype(BF16)
    dy = grad_y[...]
    y_acc[...] = x_mid + vec_row(vec, 'b_fc2')
    dh_acc[...] = jnp.zeros_like(dh_acc)
    for j in range(chunks):
        at_first(j)
        pre = dot(h_two, w_fc1[:, cols(j)]) + b_fc1[:, cols(j)]
        cdf = 0.5 + 0.5 * lax.erf(pre * (0.5 ** 0.5))
        pdf = jnp.exp(pre * pre * -0.5) * 0.3989422804014327
        act = (pre * cdf).astype(BF16)
        d_act = dot(dy, w_fc2[cols(j), :], NT)
        d_pre = d_act * (cdf + pre * pdf)
        y_acc[...] += dot(act, w_fc2[cols(j), :])
        gw_fc2[cols(j), :] += dot(act, dy, TN)
        g_b1[:, cols(j)] += col_sum(d_pre)
        d_pre = d_pre.astype(BF16)
        gw_fc1[j] += dot(h_two, d_pre, TN)
        dh_acc[...] += dot(d_pre, w_fc1[:, cols(j)], NT)
        if j > 0:
            at_last(j - 1)
    at_last(chunks - 1)
    y_out[...] = y_acc[...].astype(BF16)
    d_two = dh_acc[...]
    dy_f = dy.astype(F32)
    d_mid = dy_f + hat_bwd(d_two, x_hat, inv_std, gain)
    dmid_out[...] = d_mid
    for row, grad in enumerate((d_mid, d_two * x_hat, d_two, dy_f)):
        g_small[row:row + 1, :] += col_sum(grad)
    d_mid = d_mid.astype(BF16)
    gw_out[...] += dot(ctx_val, d_mid, TN)
    dctx_out[...] = dot(d_mid, w_out[...], NT).astype(BF16)
    at_last(chunks)

    @pl.when(step == pl.num_programs(0) - 1)
    def _():
        for j in range(chunks + 1):
            for copy in stores(j):
                copy.wait()


def whole(shape):
    return pl.BlockSpec(shape, lambda *_: (0,) * len(shape), pipeline_mode=pl.Buffered(1))


def shape_of(dims, dtype):
    return jax.ShapeDtypeStruct(dims, dtype)


def call(kernel, grid, in_specs, out_specs, out_shape, args, flops, scratch=(), name=None, collective_id=None):
    moved = sum(a.size * a.dtype.itemsize for a in args) + sum(o.size * o.dtype.itemsize for o in out_shape)
    return pl.pallas_call(
        kernel, grid=grid, in_specs=in_specs, out_specs=out_specs, out_shape=out_shape,
        scratch_shapes=list(scratch), name=name,
        compiler_params=pltpu.CompilerParams(vmem_limit_bytes=VMEM_LIMIT,
                                             dimension_semantics=('arbitrary',) * len(grid),
                                             collective_id=collective_id,
                                             has_side_effects=collective_id is not None),
        cost_estimate=pl.CostEstimate(flops=flops, bytes_accessed=moved, transcendentals=0))(*args)


def layer_compute(tokens, grad_y, vec_part, weights):
    seqs, seq_len = tokens.shape
    dim, ff = grad_y.shape[2], weights[2].shape[1]
    n_tok, pairs, half = seqs * seq_len, dim // PAIR, dim // 2
    cos, sin = rope_tables(seq_len)
    tok_seq = tokens.reshape(seqs, 1, seq_len)
    any_spec = pl.BlockSpec(memory_space=pl.ANY)
    wide = shape_of((n_tok, dim), BF16)
    wide_f32 = shape_of((n_tok, dim), F32)

    def rows_spec(rows, width=dim):
        return pl.BlockSpec((rows, width), lambda i: (i, 0))

    def wholes(*arrays):
        return [whole(a.shape) for a in arrays]

    def sems(*counts):
        return [pltpu.SemaphoreType.DMA((n,)) for n in counts]

    tile = 384
    per_seq = seq_len // tile
    table_spec = pl.BlockSpec((tile, PAIR), lambda i: (i % per_seq, 0))
    full = [shape_of((2 * w.shape[0],) + w.shape[1:], BF16) for w in weights]
    vec_shape = shape_of((2,) + vec_part.shape, BF16)
    x_in, q, k, v, vec, w_qkv, w_out, w_fc1, w_fc2 = call(
        qkv_kernel, (n_tok // tile,),
        [pl.BlockSpec((1, 1, seq_len), lambda i: (i // per_seq, 0, 0)),
         any_spec, table_spec, table_spec] + [any_spec] * 4,
        [rows_spec(tile)] * 4 + wholes(vec_shape) + [any_spec] * 4, [wide] * 4 + [vec_shape] + full,
        (tok_seq, vec_part, cos, sin) + tuple(weights),
        6 * n_tok * dim * dim,
        scratch=[pltpu.VMEM(full[0].shape, BF16), pltpu.VMEM(vec_shape.shape, BF16)]
        + [pltpu.VMEM(w.shape, BF16) for w in weights[1:]] + sems(5, 5, 9), name='qkv', collective_id=2)

    head_spec = pl.BlockSpec((seq_len, PAIR), lambda b, p: (b, p))
    tok_spec = pl.BlockSpec((1, 1, seq_len), lambda b, p: (b, 0, 0))
    lse_spec = pl.BlockSpec((1, 2, seq_len), lambda b, p: (b * pairs + p, 0, 0))
    ctx, lse = call(
        attn_fwd_kernel, (seqs, pairs), [head_spec] * 3 + [tok_spec], [head_spec, lse_spec],
        [wide, shape_of((seqs * pairs, 2, seq_len), F32)],
        (q, k, v, tok_seq), 16 * n_tok * seq_len * dim, name='attn_fwd')

    tile = 512
    pages = shape_of((ff // dim, dim, dim), F32)
    grads = [shape_of(w_out.shape, F32), pages, shape_of(w_fc2.shape, F32), shape_of((8, dim), F32),
             shape_of((1, ff), F32)]
    hidden, d_mid, d_ctx, gw_out, gw_fc1, gw_fc2, small_two, g_b1 = call(
        ffn_kernel, (n_tok // tile,), [rows_spec(tile)] * 3 + [any_spec] * 3 + wholes(vec),
        [rows_spec(tile)] * 3 + [any_spec] * 3 + wholes(*grads[3:]), [wide, wide_f32, wide] + grads,
        (ctx, x_in, grad_y.reshape(n_tok, dim), w_out, w_fc1, w_fc2, vec),
        6 * n_tok * dim * (dim + 2 * ff), scratch=[pltpu.VMEM((tile, dim), F32)] * 2 + [pltpu.VMEM(w.shape, BF16) for w in (w_out, w_fc1, w_fc2)]
        + [pltpu.VMEM(g.shape, F32) for g in grads[:3]] + [pltpu.VMEM((1, ff), F32)] + sems(2 * ff // dim + 1), name='ffn')

    blocks = (3, RING, RING, half // (3 * RING * RING), dim)
    whole_table = pl.BlockSpec((seq_len, PAIR), lambda b, p: (0, 0))
    red_shape = shape_of((3, 2) + blocks[3:], F32)
    sum_shape = shape_of((seqs * pairs, 3, PAIR), F32)
    n_sems = 2 + 12 * SCATTER_SEMS
    dq, dk, dv, b_sums, red = call(
        attn_bwd_reduce_kernel, (seqs, pairs),
        [head_spec] * 4 + [lse_spec, tok_spec, whole_table, whole_table, any_spec, any_spec],
        [head_spec] * 3 + [pl.BlockSpec((1, 3, PAIR), lambda b, p: (b * pairs + p, 0, 0))] + wholes(red_shape),
        [wide] * 3 + [sum_shape, red_shape],
        (q, k, v, d_ctx, lse, tok_seq, cos, sin, gw_fc2.reshape((2, RING) + blocks), gw_fc1.reshape((RING, 2) + blocks)),
        40 * n_tok * seq_len * dim,
        scratch=[pltpu.VMEM((RING, 2) + blocks, F32)] * 2
        + comm_temps(2, blocks[3], dim) + sems(n_sems, n_sems, 2), name='attn_bwd', collective_id=0)

    n_sems = 16 + 18 * FLOW_SEMS
    fc2, fc1, out, qkv, small_sum = call(
        qkv_bwd_reduce_kernel, (seqs,),
        [pl.BlockSpec((1, 1, seq_len), lambda i: (i, 0, 0))] + [rows_spec(seq_len)] * 5
        + wholes(w_qkv, vec, red, small_two, g_b1, b_sums) + [any_spec],
        [any_spec] * 4 + [whole((SMALL_ROWS, half))],
        [shape_of((RING,) + blocks, F32), shape_of(blocks[:-1] + (ff,), F32), shape_of(blocks, F32),
         shape_of(blocks[:-1] + (3 * dim,), F32), shape_of((SMALL_ROWS, half), F32)],
        (tok_seq, x_in, dq, dk, dv, d_mid, w_qkv, vec, red, small_two, g_b1, b_sums, gw_out.reshape((2,) + blocks)),
        12 * n_tok * dim * dim,
        scratch=[pltpu.VMEM((RING, 2) + blocks, F32), pltpu.VMEM((RING, 1) + blocks, F32)]
        + comm_temps(1, blocks[3], dim)
        + [pltpu.VMEM((RING, 2) + blocks, F32), pltpu.VMEM((2, SMALL_ROWS, half), F32),
           pltpu.VMEM((SMALL_ROWS, half), F32), pltpu.VMEM((3, RING, SMALL_ROWS, half), F32)]
        + sems(n_sems, n_sems, 10), name='qkv_bwd', collective_id=1)
    big = (qkv.reshape(half, 3 * dim), out.reshape(half, dim), fc1.reshape(half, ff), fc2.reshape(ff // 2, dim))
    return hidden.reshape(grad_y.shape), big, small_sum


RING = 4
ALL = slice(None)
DIRECT = 2
ORDERS = ('xyz', 'yzx', 'zxy')
STRIDE = {'x': 1, 'y': RING, 'z': RING * RING}
MESH_ID = pl.DeviceIdType.MESH


class Torus:
    def __init__(self):
        self.me = lax.axis_index('dp')
        self.part = lax.axis_index('fsdp')
        self.coord = {axis: self.me // stride % RING for axis, stride in STRIDE.items()}

    def at(self, axis, delta):
        return (self.coord[axis] + delta + RING) % RING

    def chip(self, axis, delta):
        return {'dp': self.me + (self.at(axis, delta) - self.coord[axis]) * STRIDE[axis]}

    def partner(self):
        return {'fsdp': 1 - self.part}

    def greet(self):
        barrier = pltpu.get_barrier_semaphore()
        peers = [self.partner()] + [self.chip(axis, delta) for axis in 'xyz' for delta in (1, -1, 2)]
        for peer in peers:
            pl.semaphore_signal(barrier, inc=1, device_id=peer, device_id_type=MESH_ID)
        pl.semaphore_wait(barrier, len(peers))


class Flow:
    def __init__(self, torus, order, sign, view, temp_view, grads, sums, temps, sends, recvs, base):
        self.torus, self.order, self.sign = torus, order, sign
        self.view, self.temp_view = view, temp_view
        self.grads, self.sums, self.temps = grads, sums, temps
        self.sends, self.recvs, self.base = sends, recvs, base
        self.used = []

    def route(self, slot):
        level, kind = slot % 9 // 3, slot % 3
        sign = self.sign
        if slot < 9:
            target = self.temp_view(self.temps, level, kind)
            if kind == 2 and level != DIRECT:
                return self.temp_view(self.temps, level, 0), target, level, sign
            delta = (2, -sign, sign)[kind]
            return self.view(self.grads, self.place(level, delta)), target, level, delta if level == DIRECT or kind else sign
        if kind == 2 and level != DIRECT:
            block = self.view(self.sums, self.place(level, -sign))
            return block, block, level, sign
        target = self.view(self.sums, self.place(level + 1))
        source = self.final(self) if level == DIRECT else target
        return source, target, level, (sign, -sign, 2)[kind]

    def copy(self, slot):
        src, dst, level, delta = self.route(slot)
        return pltpu.make_async_remote_copy(
            src_ref=src, dst_ref=dst, send_sem=self.sends.at[self.base + slot],
            recv_sem=self.recvs.at[self.base + slot],
            device_id=self.torus.chip(self.order[level], delta), device_id_type=MESH_ID)

    def start(self, slot):
        self.used.append(slot)
        self.copy(slot).start()

    def wait(self, slot):
        self.copy(slot).wait_recv()

    def place(self, level, delta=None):
        own = [self.torus.coord[axis] for axis in self.order[:level]]
        return tuple(own) + (() if delta is None else (self.torus.at(self.order[level], delta),))

    def start_level(self, first, level):
        for kind in range(3 if level == DIRECT else 2):
            self.start(first + kind)

    def wait_level(self, first, level):
        for kind in range(0 if level == DIRECT else 1, 3):
            self.wait(first + kind)

    def scatter_start(self, level):
        self.start_level(level * 3, level)

    def scatter_mid(self, level):
        if level == DIRECT:
            return
        self.wait(level * 3)
        relay = self.temp_view(self.temps, level, 0)
        relay[...] = relay[...] + self.view(self.grads, self.place(level, self.sign))[...]
        self.start(level * 3 + 2)

    def scatter_end(self, level):
        self.wait_level(level * 3, level)
        mine = self.view(self.grads, self.place(level, 0))
        total = mine[...]
        for kind in range(0 if level == DIRECT else 1, 3):
            total = total + self.temp_view(self.temps, level, kind)[...]
        mine[...] = total

    def gather_start(self, level):
        if level == DIRECT:
            self.view(self.sums, self.place(3))[...] = self.final(self)[...]
        self.start_level(9 + level * 3, level)

    def gather_mid(self, level):
        if level == DIRECT:
            return
        self.wait(9 + level * 3)
        self.start(11 + level * 3)

    def gather_end(self, level):
        self.wait_level(9 + level * 3, level)

    def scatter_next(self, level):
        self.scatter_end(level)
        if level == DIRECT:
            self.gather_start(level)
        else:
            self.scatter_start(level + 1)

    def gather_next(self, level):
        self.gather_end(level)
        self.gather_start(level - 1)

    def finish(self):
        for slot in self.used:
            self.copy(slot).wait_send()


FLOW_SEMS = 18
SCATTER_SEMS = 9


def own_block(flow):
    return flow.view(flow.grads, flow.place(3))


def make_flows(torus, width, grads, sums, temps, sends, recvs, base, group=ALL, temp_group=ALL, final=own_block,
               spacing=FLOW_SEMS, pieces=None):
    half = width // 2
    flows = []
    for first, size in pieces or ((0, half),):
        for color, order, side in [(color, order, side) for color, order in enumerate(ORDERS) for side in range(2)]:
            sign = 1 - 2 * side
            lanes = pl.ds(side * half + first, size)

            def view(ref, place, color=color, lanes=lanes):
                rest = place[1:] + (ALL,) * (4 - len(place))
                return ref.at[(place[0], group if ref is grads else ALL, color) + rest + (lanes,)]

            def temp_view(refs, level, kind, color=color, lanes=lanes):
                return refs[level].at[(kind, temp_group, color) + (ALL,) * (3 - level) + (lanes,)]

            flow = Flow(torus, order, sign, view, temp_view, grads, sums, temps, sends, recvs,
                        base + len(flows) * spacing)
            flow.final, flow.color, flow.lanes = final, color, lanes
            flows.append(flow)
    return flows


def each(flows, name, level):
    for flow in flows:
        getattr(flow, name)(level)


def comm_temps(groups, rows, dim):
    return [pltpu.VMEM((3, groups, 3) + (RING,) * (2 - level) + (rows, dim), F32) for level in range(3)]


PLAN = ('b', '', 'e0', '', 'e1', 'm00', '', 'm10', 'a00', 'm01 a10', 'a01 m11', 'a11', 'a02 a12')


def attn_bwd_reduce_kernel(q, k, v, d_ctx, lse, tok_seq, cos, sin, fc2, fc1, dq_out, dk_out, dv_out, sums_out, red,
                           grads, other_sum, temp0, temp1, temp2, sends, recvs, local):
    torus = Torus()
    step = pl.program_id(0) * pl.num_programs(1) + pl.program_id(1)
    sets = [make_flows(torus, grads.shape[-1], grads, None, (temp0, temp1, temp2), sends, recvs,
                       2 + n * 6 * SCATTER_SEMS, group=pl.ds(n, 1), temp_group=pl.ds(n, 1), spacing=SCATTER_SEMS)
            for n in range(2)]
    sources = (lambda i: fc2.at[i], lambda i: fc1.at[:, i])

    def remote(n):
        return pltpu.make_async_remote_copy(
            src_ref=sources[n](1 - torus.part), dst_ref=other_sum.at[:, n], send_sem=sends.at[n], recv_sem=recvs.at[n],
            device_id=torus.partner(), device_id_type=MESH_ID)

    def mine(n):
        return pltpu.make_async_copy(sources[n](torus.part), grads.at[:, n], local.at[n])

    def begin():
        torus.greet()
        for n in range(2):
            remote(n).start()
            mine(n).start()

    def enter(n):
        remote(n).wait_recv()
        mine(n).wait()

        @pl.loop(0, RING)
        def _(page):
            grads[page, n] = grads[page, n] + other_sum[page, n]
        each(sets[n], 'scatter_start', 0)

    def mid(n, level):
        each(sets[n], 'scatter_mid', level)

    def after(n, level):
        each(sets[n], 'scatter_next' if level < 2 else 'scatter_end', level)

    actions = {'b': begin, 'e': enter, 'm': mid, 'a': after}

    def perform(words):
        for word in words.split():
            actions[word[0]](*(int(number) for number in word[1:]))

    for at_step, words in enumerate(PLAN[:-1]):
        pl.when(step == at_step)(functools.partial(perform, words))

    attn_bwd_kernel(q, k, v, d_ctx, lse, tok_seq, cos, sin, dq_out, dk_out, dv_out, sums_out)

    @pl.when(step == len(PLAN) - 2)
    def _():
        perform(PLAN[-1])
        for n, flows in enumerate(sets):
            for flow in flows:
                red[flow.color, n:n + 1, :, flow.lanes] = own_block(flow)[...]
                flow.finish()
            remote(n).wait_send()


def qkv_bwd_reduce_kernel(tok_seq, x_in, dq, dk, dv, d_mid, w_qkv, vec, red, small_two, g_b1, b_sums,
                          gw_out, fc2_sum, fc1_sum, out_sum, qkv_sum, small_sum,
                          grads, sums, temp0, temp1, temp2, sums_ab, small, small_other, small_slots,
                          sends, recvs, local):
    torus = Torus()
    step = pl.program_id(0)
    last = pl.num_programs(0) - 1
    dim = x_in.shape[1]
    half = dim // 2
    part = torus.part

    def final(flow):
        return red.at[flow.color, :, :, flow.lanes]

    gathers = make_flows(torus, dim, None, sums_ab, None, sends, recvs, 16, final=final)
    flows = make_flows(torus, dim, grads, sums, (temp0, temp1, temp2), sends, recvs, 16 + 6 * FLOW_SEMS,
                       group=pl.ds(part, 1), pieces=((0, 2 * PAIR), (2 * PAIR, PAIR)))

    def load_out():
        return pltpu.make_async_copy(gw_out, grads.at[0], local.at[0])

    def middle_hook():
        each(gathers, 'gather_mid', 1)
        load_out().wait()

    hooks = ((0, 1, lambda: each(gathers, 'gather_next', 2)), (1, 0, middle_hook),
             (1, 1, lambda: each(gathers, 'gather_next', 1)))

    def pair_copy(page):
        return pltpu.make_async_remote_copy(
            src_ref=grads.at[page, 1 - part], dst_ref=sums.at[page, 0], send_sem=sends.at[1 + page],
            recv_sem=recvs.at[1 + page], device_id=torus.partner(), device_id_type=MESH_ID)

    @pl.when(step == 0)
    def _():
        torus.greet()
        load_out().start()
        each(gathers, 'gather_start', 2)
        small[...] = jnp.zeros_like(small)
        for page in range(1, RING):
            grads[page] = jnp.zeros(grads.shape[1:], F32)

    x_hat, inv_std = hat_of(x_in[...].astype(F32))
    gain = vec_row(vec, 'ln1_gain')
    h_one = (x_hat * gain + vec_row(vec, 'ln1_bias')).astype(BF16)
    d_one = None
    for index, ref in enumerate((dq, dk, dv)):
        for at_step, at_index, hook in hooks:
            if at_index == index:
                pl.when(step == at_step)(hook)
        cols = slice(index * dim, (index + 1) * dim)
        d_part = ref[...]
        grads[index + 1] += dot(h_one, d_part, TN).reshape(grads.shape[1:])
        new = dot(d_part, w_qkv[:, cols], NT)
        pl.when(step == last)(pair_copy(index).start)
        d_one = new if index == 0 else d_one + new
    g_rows = jnp.concatenate([col_sum(d_one * x_hat), col_sum(d_one)], axis=0)
    d_in = d_mid[...] + hat_bwd(d_one, x_hat, inv_std, gain)
    scale, _ = seq_counts(tok_seq[0])
    one_hot = live_one_hot(tok_seq[0], EMB_ROWS)
    high = d_in.astype(BF16)
    low = (d_in - high.astype(F32)).astype(BF16)
    g_emb = (dot(one_hot, high) + dot(one_hot, low)) * scale
    for side in range(2):
        lanes = slice(side * half, (side + 1) * half)
        small[side, :EMB_ROWS, :] += g_emb[:, lanes]
        small[side, EMB_ROWS:EMB_ROWS + 2, :] += g_rows[:, lanes]

    @pl.when(step == last)
    def _():
        pair_copy(RING - 1).start()
        pairs = dim // PAIR
        per_pair = [b_sums[p] for p in range(pairs)]
        for b in range(1, b_sums.shape[0] // pairs):
            per_pair = [per_pair[p] + b_sums[b * pairs + p] for p in range(pairs)]
        b_qkv = jnp.concatenate([per_pair[p][i:i + 1] for i in range(3) for p in range(pairs)], axis=1)
        for side in range(2):
            row = EMB_ROWS + 2
            small[side, row:row + 4, :] = small_two[:4, side * half:(side + 1) * half]
            row += 4
            for grad in (b_qkv, g_b1[...]):
                base = side * (grad.shape[1] // 2)
                for i in range(grad.shape[1] // dim):
                    small[side, row:row + 1, :] = grad[:, base + i * half:base + (i + 1) * half]
                    row += 1
        small_copy = pltpu.make_async_remote_copy(
            src_ref=small.at[1 - part], dst_ref=small_other, send_sem=sends.at[0], recv_sem=recvs.at[0],
            device_id=torus.partner(), device_id_type=MESH_ID)
        small_copy.start()
        started = [small_copy] + [pair_copy(page) for page in range(RING)]

        def small_start(level, value):
            axis = ORDERS[0][level]
            here = torus.coord[axis]
            small_slots[level, here] = value
            slot = small_slots.at[level, here]
            copies = [pltpu.make_async_remote_copy(
                src_ref=slot, dst_ref=slot, send_sem=sends.at[5 + level * 3 + n], recv_sem=recvs.at[5 + level * 3 + n],
                device_id=torus.chip(axis, delta), device_id_type=MESH_ID) for n, delta in enumerate((1, -1, 2))]
            for copy in copies:
                copy.start()
            started.extend(copies)
            return copies

        def small_end(level, copies):
            for copy in copies:
                copy.wait_recv()
            return ((small_slots[level, 0] + small_slots[level, 1]) + small_slots[level, 2]) + small_slots[level, 3]

        small_copy.wait_recv()
        small_copies = small_start(0, small[part] + small_other[...])
        for page in range(RING):
            started[1 + page].wait_recv()

            @pl.loop(0, 3)
            def _(i):
                grads[page, part, i] = grads[page, part, i] + sums[page, 0, i]
        each(flows, 'scatter_start', 0)
        each(gathers, 'gather_mid', 0)
        for level in range(3):
            each(flows, 'scatter_mid', level)
            total = small_end(level, small_copies)
            if level < 2:
                small_copies = small_start(level + 1, total)
            each(flows, 'scatter_next', level)
        small_sum[...] = total
        each(gathers, 'gather_end', 0)
        stores = [pltpu.make_async_copy(sums_ab.at[:, 0], fc2_sum, local.at[1])]
        for page in range(RING):
            lanes = pl.ds(page * dim, dim)
            stores.append(pltpu.make_async_copy(sums_ab.at[page, 1], fc1_sum.at[:, :, :, :, lanes], local.at[2 + page]))
        for store in stores:
            store.start()
        each(flows, 'gather_mid', 2)
        for level in (1, 0):
            each(flows, 'gather_next', level + 1)
            each(flows, 'gather_mid', level)
        each(flows, 'gather_end', 0)
        tail = [pltpu.make_async_copy(sums.at[0, 0], out_sum, local.at[6])]
        for page in range(3):
            tail.append(pltpu.make_async_copy(
                sums.at[page + 1, 0], qkv_sum.at[:, :, :, :, pl.ds(page * dim, dim)], local.at[7 + page]))
        for store in tail:
            store.start()
        for copy in started:
            copy.wait_send()
        for flow in gathers + flows:
            flow.finish()
        for store in stores + tail:
            store.wait()


def solution(mesh):
    row_spec = P(('dp', 'fsdp'), None)
    act_spec = P(('dp', 'fsdp'), None, None)
    param_specs = (P(None, 'fsdp'),) + (P('fsdp'),) * 12

    def local_step(tokens, grad_y, *shards):
        (embedding, ln1_gain, ln1_bias, w_qkv, b_qkv, w_out, b_out,
         ln2_gain, ln2_bias, w_fc1, b_fc1, w_fc2, b_fc2) = shards
        vectors = (ln1_gain, ln1_bias, b_out, ln2_gain, ln2_bias, b_fc2, b_qkv, b_fc1)
        vocab, width = embedding.shape
        rows = [vec[first:first + width] for vec in vectors for first in range(0, vec.size, width)]
        at_row = jnp.asarray(np.indices((SMALL_ROWS, width))[0], jnp.int32)
        vec_part = jnp.pad(embedding, ((0, SMALL_ROWS - vocab), (0, 0)))
        for index, row in enumerate(rows):
            vec_part = jnp.where(at_row == VEC_ROW + index, row[None, :], vec_part)
        hidden, big, small_sum = layer_compute(tokens, grad_y, vec_part, (w_qkv, w_out, w_fc1, w_fc2))
        g_w_qkv, g_w_out, g_w_fc1, g_w_fc2 = big
        g_embedding = small_sum[:vocab]
        start = EMB_ROWS
        vec_grads = []
        for vec in vectors:
            stop = start + vec.size // width
            vec_grads.append(small_sum[start:stop].reshape(-1))
            start = stop
        (g_ln1_gain, g_ln1_bias, g_b_out, g_ln2_gain, g_ln2_bias, g_b_fc2, g_b_qkv, g_b_fc1) = vec_grads
        return (hidden, g_embedding, g_ln1_gain, g_ln1_bias, g_w_qkv, g_b_qkv, g_w_out, g_b_out,
                g_ln2_gain, g_ln2_bias, g_w_fc1, g_b_fc1, g_w_fc2, g_b_fc2)

    return jax.shard_map(local_step, mesh=mesh, in_specs=(row_spec, act_spec) + param_specs,
                         out_specs=(act_spec,) + param_specs, check_vma=False)
```
